512 devices in a mesh: groups: 2 (over y), date: 32 (over z, core), tile: 8 (over x).
Axes of the slice: x: 8, y: 2, z: 16, core: 2. Of those that a mesh axis runs over, the one named last changes fastest.
The devices are a block of a 8x8x16 slice.
Arguments:
- acquired: float32 [2, 256, 256, 128], P(None, 'date', ('groups', 'tile')), parts along dimension 2, may hold values from -10 to 10, as said below
Outputs:
- coherence: float32 [2, 4, 256, 8, 256, 128], P(None, None, 'date', None, ('groups', 'tile')), parts along dimension 4
The draws below stay inside these ranges and needn't reach their ends.
There are 2 independent parts, one for each index of `groups`. The reference program is written for one: setup_inputs(seed, part) draws one part's arguments, and reference() takes and returns one part's arrays. A program takes and returns all parts, laid end to end along the dimension named above; each array names one. Nothing has to cross between parts.
Inputs may be any that keep to these rules, and one draw needn't show every extreme that they name: `acquired`: every pixel's magnitude, the square root of the sum of its two parts squared, lies between 0.1 and 10.
All inputs are finite; a program needn't handle non-finite values.
Results may differ from the reference program's by a relative error of at most 0.000058.
Values sent between devices are 32-bit elements; how exact they have to be, the bound alone decides.
A program may use at most 64 MiB of HBM per device.

```python
import math
import jax
import jax.numpy as jnp
from jax import lax

DATE_DEV = 8
SHIFTS = 4
COLS = 128
DATES = 256
ROWS = 128


def draw_acquired(key, part):
    key_mag = jax.random.fold_in(key, 11)
    key_common = jax.random.fold_in(key, 12)
    key_ramp = jax.random.fold_in(key, 13)
    key_speckle = jax.random.fold_in(key, 14)
    lowest = 0.3
    highest = 3.0
    spread = 0.8
    magnitude = jnp.exp(jax.random.uniform(key_mag, (DATES, ROWS, COLS), jnp.float32, math.log(lowest), math.log(highest)))
    common_phase = jax.random.uniform(key_common, (1, ROWS, COLS), jnp.float32, -math.pi, math.pi)
    date_ramp = jax.random.uniform(key_ramp, (DATES, 1, 1), jnp.float32, -0.5, 0.5) * jnp.arange(COLS, dtype=jnp.float32)[None, None, :]
    speckle = spread * jax.random.normal(key_speckle, (DATES, ROWS, COLS), jnp.float32)
    phases = common_phase + date_ramp + speckle
    return jnp.stack([magnitude * jnp.cos(phases), magnitude * jnp.sin(phases)]).astype(jnp.float32)


def setup_inputs(seed: int = 0, part: int = 0) -> dict:
    key_list = jax.random.split(jax.random.key(seed), 2)
    part_keys = jax.random.split(jax.random.fold_in(key_list[1], part), 2)
    acquired = draw_acquired(jax.random.fold_in(jax.random.fold_in(key_list[1], part), 71), part)
    return {"acquired": acquired}


row_reach = 5
col_reach = 2

def box_sum(values_in):
    height = values_in.shape[-2]
    breadth = values_in.shape[-1]
    widths = [(0, 0)] * (values_in.ndim - 2) + [(row_reach, row_reach), (col_reach, col_reach)]
    padded = jnp.pad(values_in, widths)
    summed = padded[..., 0:height, :]
    for shift_at in range(1, 2 * row_reach + 1):
        summed = summed + padded[..., shift_at:shift_at + height, :]
    result = summed[..., 0:breadth]
    for shift_at in range(1, 2 * col_reach + 1):
        result = result + summed[..., shift_at:shift_at + breadth]
    return result

def reference(acquired):
    dates_all = acquired.shape[1]
    height = acquired.shape[2]
    breadth = acquired.shape[3]
    nblocks = dates_all // DATE_DEV
    power = box_sum(acquired[0] * acquired[0] + acquired[1] * acquired[1])
    blocks = []
    for offset in range(SHIFTS):
        partner = jnp.roll(acquired, -offset * DATE_DEV, axis=1)
        partner_power = jnp.roll(power, -offset * DATE_DEV, axis=0)
        anchor = acquired.reshape(2, nblocks, DATE_DEV, 1, height, breadth)
        other = partner.reshape(2, nblocks, 1, DATE_DEV, height, breadth)
        cross_re = box_sum(anchor[0] * other[0] + anchor[1] * other[1])
        cross_im = box_sum(anchor[1] * other[0] - anchor[0] * other[1])
        inverse = lax.rsqrt(power.reshape(nblocks, DATE_DEV, 1, height, breadth) * partner_power.reshape(nblocks, 1, DATE_DEV, height, breadth))
        block = jnp.stack([cross_re * inverse, cross_im * inverse])
        blocks.append(block.reshape(2, dates_all, DATE_DEV, height, breadth))
    return jnp.stack(blocks, axis=1)
```

```python
import functools

import jax
import jax.numpy as jnp
from jax import lax
from jax.experimental import pallas as pl
from jax.experimental.pallas import tpu as pltpu
from jax.sharding import PartitionSpec as P

SHIFTS = 4
row_reach = 5
col_reach = 2
EDGE = 8
MESH = pl.DeviceIdType.MESH


def when(*conditions):
    return pl.when(functools.reduce(jnp.logical_and, conditions))


def exchange_kernel(
    dates, tiles, mine, core, above, below, relay,
    send, got_core, got_above, got_below, relay_send, relay_got, ready,
):
    me = lax.axis_index("date")
    tile = lax.axis_index("tile")
    height = mine.shape[2]
    middle = dates * 9 // 16
    origin = me - middle
    relays = (origin >= 0) & (origin < SHIFTS - 1)
    first = me < SHIFTS - 1

    def there(side):
        return (tile + side >= 0) & (tile + side < tiles)

    routes = [(step, side) for step in range(SHIFTS) for side in (1, -1, 0) if (step, side) != (0, 0)]

    def piece(step, side, source):
        if side == 0:
            return source, core.at[step - 1], got_core.at[step - 1]
        if side == 1:
            return source.at[:, :, pl.ds(height - EDGE, EDGE), :], above.at[step], got_above.at[step]
        return source.at[:, :, pl.ds(0, EDGE), :], below.at[step], got_below.at[step]

    def copy(step, side, source, date, sems):
        src, dst, got = piece(step, side, source)
        return pltpu.make_async_remote_copy(
            src_ref=src, dst_ref=dst, send_sem=sems.at[step, side + 1], recv_sem=got,
            device_id={"date": date, "tile": tile + side}, device_id_type=MESH,
        )

    barrier = pltpu.get_barrier_semaphore()
    count = jnp.int32(0)
    for step, side in routes:
        @when(there(side))
        def _():
            straight = me + step < dates

            @pl.when(straight)
            def _():
                pl.semaphore_signal(
                    barrier, inc=1, device_id={"date": me + step, "tile": tile + side}, device_id_type=MESH)

        count += (there(-side) & (me - step >= 0)).astype(jnp.int32)
        count += (there(side) & (me + step >= dates)).astype(jnp.int32)
    for step, side in routes:
        @when(relays, step > origin, there(side))
        def _():
            pl.semaphore_signal(
                barrier, inc=1, device_id={"date": dates + origin - step, "tile": tile + side}, device_id_type=MESH)

    @pl.when(first)
    def _():
        pl.semaphore_signal(barrier, inc=1, device_id={"date": me + middle, "tile": tile}, device_id_type=MESH)

    count += relays.astype(jnp.int32)
    pl.semaphore_wait(barrier, count)

    for step, side in routes:
        @when(there(side), me - step >= 0)
        def _():
            copy(step, side, mine, me - step, send).start()

    @pl.when(relays)
    def _():
        pl.semaphore_signal(ready, inc=1, device_id={"date": origin, "tile": tile}, device_id_type=MESH)

    for step, side in routes:
        @when(there(side), me + step >= dates)
        def _():
            pl.semaphore_signal(
                ready, inc=1, device_id={"date": me + step - dates + middle, "tile": tile + side}, device_id_type=MESH)

    @pl.when(tile == 0)
    def _():
        above[...] = jnp.zeros_like(above)

    @pl.when(tile == tiles - 1)
    def _():
        below[...] = jnp.zeros_like(below)

    def to_relay():
        return pltpu.make_async_remote_copy(
            src_ref=mine, dst_ref=relay, send_sem=relay_send.at[0, 1], recv_sem=relay_got,
            device_id={"date": me + middle, "tile": tile}, device_id_type=MESH,
        )

    @pl.when(first)
    def _():
        pl.semaphore_wait(ready, 1)
        to_relay().start()

    @pl.when(relays)
    def _():
        count = jnp.int32(0)
        for step, side in routes:
            count += ((step > origin) & there(side)).astype(jnp.int32)
        pl.semaphore_wait(ready, count)
        to_relay().wait_recv()
        for step, side in routes:
            if step:
                @when(step > origin, there(side))
                def _():
                    copy(step, side, relay, dates + origin - step, relay_send).start()

    for step, side in reversed(routes):
        @pl.when(there(-side))
        def _():
            copy(step, side, mine, me, send).wait_recv()

    for step, side in routes:
        @when(there(side), me - step >= 0)
        def _():
            copy(step, side, mine, me - step, send).wait_send()

    @pl.when(first)
    def _():
        to_relay().wait_send()

    for step, side in routes:
        if step:
            @when(relays, step > origin, there(side))
            def _():
                copy(step, side, relay, dates + origin - step, relay_send).wait_send()


def exchange(acquired, dates, tiles):
    parts, block, height, breadth = acquired.shape
    shape = (parts, block, height, breadth)
    edge = (SHIFTS, parts, block, EDGE, breadth)
    return pl.pallas_call(
        functools.partial(exchange_kernel, dates, tiles),
        out_shape=(
            jax.ShapeDtypeStruct((SHIFTS - 1,) + shape, jnp.float32),
            jax.ShapeDtypeStruct(edge, jnp.float32),
            jax.ShapeDtypeStruct(edge, jnp.float32),
        ),
        in_specs=[pl.BlockSpec(memory_space=pl.ANY)],
        out_specs=(pl.BlockSpec(memory_space=pltpu.VMEM),) * 3,
        scratch_shapes=[
            pltpu.VMEM(shape, jnp.float32),
            pltpu.SemaphoreType.DMA((SHIFTS, 3)),
            pltpu.SemaphoreType.DMA((SHIFTS - 1,)),
            pltpu.SemaphoreType.DMA((SHIFTS,)),
            pltpu.SemaphoreType.DMA((SHIFTS,)),
            pltpu.SemaphoreType.DMA((SHIFTS, 3)),
            pltpu.SemaphoreType.DMA,
            pltpu.SemaphoreType.REGULAR,
        ],
        compiler_params=pltpu.CompilerParams(
            collective_id=0, has_side_effects=True, vmem_limit_bytes=8 << 20),
        name="exchange",
    )(acquired)


def window_sums(rows, height):
    width = 2 * row_reach + 1
    sums = [None] * height
    start = 0
    while start < height:
        size = min(width, height - start)
        last = start + width - 1
        tail = rows[last]
        tails = {last: tail}
        for row in range(last - 1, start - 1, -1):
            tail = tail + rows[row]
            tails[row] = tail
        sums[start] = tails[start]
        head = None
        for row in range(start + 1, start + size):
            new = rows[row + width - 1]
            head = new if head is None else head + new
            sums[row] = tails[row] + head
        start += size
    return sums


def coherence_kernel(
    mine, core, above, below, band, out, parts, sums, power, scale, staged, done,
):
    block, height = out.shape[2], out.shape[4]
    breadth = out.shape[5]
    rows = height + 2 * row_reach

    def split_box(values):
        high = values.astype(jnp.bfloat16)
        low = (values - high.astype(jnp.float32)).astype(jnp.bfloat16)
        return jnp.dot(jnp.concatenate([high, low], axis=1), band[...], preferred_element_type=jnp.float32)

    def by_date(ref, part):
        tiles = []
        for date in range(block):
            for at in range(0, height, 8):
                tiles.append(ref[part, pl.ds(at * block + date, 8, stride=block), :])
        return jnp.concatenate(tiles, axis=0)

    for step in range(SHIFTS):
        for part in range(2):
            for row in range(rows):
                if row < row_reach:
                    value = above[step, part, pl.ds(EDGE - row_reach + row, block, stride=EDGE), :]
                elif row < row_reach + height:
                    at = pl.ds(row - row_reach, block, stride=height)
                    value = mine[part, at, :] if step == 0 else core[step - 1, part, at, :]
                else:
                    value = below[step, part, pl.ds(row - row_reach - height, block, stride=EDGE), :]
                parts[step, part, row] = value

    for step in range(SHIFTS):
        squares = [parts[step, 0, row] * parts[step, 0, row] + parts[step, 1, row] * parts[step, 1, row] for row in range(rows)]
        for row, value in enumerate(window_sums(squares, height)):
            power[0, row * block:(row + 1) * block, :] = value
        boxed = split_box(by_date(power, 0))
        scale[step] = lax.rsqrt(boxed).reshape(block, height, breadth)

    def anchor(part, row, date):
        return jnp.broadcast_to(parts[0, part, row, pl.ds(date, 1), :], (block, parts.shape[-1]))

    def cross(step):
        for date in range(block):
            real, imag = [], []
            for row in range(rows):
                first_re, first_im = anchor(0, row, date), anchor(1, row, date)
                second_re, second_im = parts[step, 0, row], parts[step, 1, row]
                real.append(first_re * second_re + first_im * second_im)
                imag.append(first_im * second_re - first_re * second_im)
            for part, values in ((0, real), (1, imag)):
                for row, value in enumerate(window_sums(values, height)):
                    sums[date, part, row * block:(row + 1) * block, :] = value
        for date in range(block):
            weight = scale[0, date][None] * scale[step]
            for part in range(2):
                boxed = split_box(by_date(sums.at[date], part))
                staged[step, part, date] = boxed.reshape(block, height, breadth) * weight

    def copy_out(step):
        return pltpu.make_async_copy(staged.at[step], out.at[:, step], done.at[step])

    @pl.loop(0, SHIFTS)
    def _(step):
        cross(step)
        copy_out(step).start()

    @pl.loop(0, SHIFTS)
    def _(step):
        copy_out(step).wait()


def coherence(mine, core, above, below):
    parts, block, height, breadth = mine.shape
    left = lax.broadcasted_iota(jnp.int32, (2 * breadth, breadth), 0) % breadth
    right = lax.broadcasted_iota(jnp.int32, (2 * breadth, breadth), 1)
    band = (jnp.abs(left - right) <= col_reach).astype(jnp.bfloat16)
    rows = height + 2 * row_reach
    return pl.pallas_call(
        coherence_kernel,
        out_shape=jax.ShapeDtypeStruct((2, SHIFTS, block, block, height, breadth), jnp.float32),
        in_specs=[pl.BlockSpec(memory_space=pltpu.VMEM)] * 5,
        out_specs=pl.BlockSpec(memory_space=pl.ANY),
        scratch_shapes=[
            pltpu.VMEM((SHIFTS, 2, rows, block, breadth), jnp.float32),
            pltpu.VMEM((block, 2, height * block, breadth), jnp.float32),
            pltpu.VMEM((1, height * block, breadth), jnp.float32),
            pltpu.VMEM((SHIFTS, block, height, breadth), jnp.float32),
            pltpu.VMEM((SHIFTS, 2, block, block, height, breadth), jnp.float32),
            pltpu.SemaphoreType.DMA((SHIFTS,)),
        ],
        compiler_params=pltpu.CompilerParams(vmem_limit_bytes=24 << 20),
        name="coherence",
    )(
        mine.reshape(parts, block * height, breadth),
        core.reshape(SHIFTS - 1, parts, block * height, breadth),
        above.reshape(SHIFTS, parts, block * EDGE, breadth),
        below.reshape(SHIFTS, parts, block * EDGE, breadth),
        band,
    )


def solution(mesh):
    def on_device(acquired):
        core, above, below = exchange(acquired, mesh.shape["date"], mesh.shape["tile"])
        return coherence(acquired, core, above, below)

    in_specs = (P(None, "date", ("groups", "tile"), None),)
    out_specs = P(None, None, "date", None, ("groups", "tile"), None)
    return jax.shard_map(
        on_device, mesh=mesh, in_specs=in_specs, out_specs=out_specs, check_vma=False
    )
```

```python
import functools

import jax
import jax.numpy as jnp
from jax import lax
from jax.experimental import pallas as pl
from jax.experimental.pallas import tpu as pltpu
from jax.sharding import PartitionSpec as P

SHIFTS = 4
row_reach = 5
col_reach = 2
EDGE = 8
MESH = pl.DeviceIdType.MESH


def when(*conditions):
    return pl.when(functools.reduce(jnp.logical_and, conditions))


def exchange_kernel(
    dates, tiles, mine, own, core, above, below, relay,
    send, got_own, got_core, got_above, got_below, relay_send, relay_got, late_send, ready, late_ready,
):
    me = lax.axis_index("date")
    tile = lax.axis_index("tile")
    height = mine.shape[2]
    near, far = dates * 5 // 16, dates * 3 // 4
    near_block, far_block = me - near, me - far
    starts = me < SHIFTS
    is_near = (near_block >= 0) & (near_block < SHIFTS)
    is_far = (far_block >= 0) & (far_block < SHIFTS - 1)

    def there(side):
        return (tile + side >= 0) & (tile + side < tiles)

    def is_first(date, at):
        return (date == 0) & (at == 0)

    first = is_first(me, tile)
    routes = [(step, side) for step in range(SHIFTS) for side in (1, -1, 0) if (step, side) != (0, 0)]
    late = [(step, side) for step, side in routes if side < 1]

    def signal(semaphore, date, side=0):
        pl.semaphore_signal(
            semaphore, inc=1, device_id={"date": date, "tile": tile + side}, device_id_type=MESH)

    def piece(step, side, source):
        if side == 0:
            return source, core.at[step - 1], got_core.at[step - 1]
        if side == 1:
            return source.at[:, :, pl.ds(height - EDGE, EDGE), :], above.at[step], got_above.at[step]
        return source.at[:, :, pl.ds(0, EDGE), :], below.at[step], got_below.at[step]

    def copy(step, side, source, date, sems):
        src, dst, got = piece(step, side, source)
        return pltpu.make_async_remote_copy(
            src_ref=src, dst_ref=dst, send_sem=sems.at[step, side + 1], recv_sem=got,
            device_id={"date": date, "tile": tile + side}, device_id_type=MESH,
        )

    def straight(step, side):
        return there(side) & (me >= step) & ~is_first(me - step, tile + side)

    def around(step, side):
        return is_far & (step > far_block) & there(side)

    def to_first(step, side):
        return is_near & (near_block == step) & (tile + side == 0)

    barrier = pltpu.get_barrier_semaphore()
    count = jnp.int32(0)
    for step, side in routes:
        @when(there(side), me + step < dates, ~first)
        def _():
            signal(barrier, me + step, side)

        count += straight(step, side).astype(jnp.int32)
        count += (there(side) & (me + step >= dates)).astype(jnp.int32)

        @pl.when(around(step, side))
        def _():
            signal(barrier, dates + far_block - step, side)

    for step, side in late:
        count += (first & there(-side)).astype(jnp.int32)

        @pl.when(to_first(step, side))
        def _():
            signal(barrier, 0, side)

    @pl.when(starts)
    def _():
        signal(barrier, me + near)

    @when(is_near, near_block < SHIFTS - 1)
    def _():
        signal(barrier, near_block + far)

    count += is_near.astype(jnp.int32) + is_far.astype(jnp.int32)
    pl.semaphore_wait(barrier, count)

    for step, side in routes:
        @pl.when(straight(step, side))
        def _():
            copy(step, side, mine, me - step, send).start()

    keep = pltpu.make_async_copy(mine, own, got_own)
    keep.start()

    @pl.when(is_near)
    def _():
        signal(ready, near_block)

    @pl.when(is_far)
    def _():
        signal(ready, far_block + near)

    for step, side in routes:
        @when(there(side), me + step >= dates)
        def _():
            signal(ready, me + step - dates + far, side)

    for step, side in late:
        @when(first, there(-side))
        def _():
            signal(late_ready, step + near, -side)

    @pl.when(tile == 0)
    def _():
        above[...] = jnp.zeros_like(above)

    @pl.when(tile == tiles - 1)
    def _():
        below[...] = jnp.zeros_like(below)

    def to_relay(source, date):
        return pltpu.make_async_remote_copy(
            src_ref=source, dst_ref=relay, send_sem=relay_send.at[0, 1], recv_sem=relay_got,
            device_id={"date": date, "tile": tile}, device_id_type=MESH,
        )

    @pl.when(starts)
    def _():
        pl.semaphore_wait(ready, 1)
        to_relay(mine, me + near).start()

    @pl.when(is_near | is_far)
    def _():
        to_relay(mine, me).wait_recv()

    @when(is_near, near_block < SHIFTS - 1)
    def _():
        pl.semaphore_wait(ready, 1)
        to_relay(relay, near_block + far).start()

    for step, side in late:
        @pl.when(to_first(step, side))
        def _():
            pl.semaphore_wait(late_ready, 1)
            copy(step, side, relay, 0, late_send).start()

    @pl.when(is_far)
    def _():
        count = jnp.int32(0)
        for step, side in routes:
            count += around(step, side).astype(jnp.int32)
        pl.semaphore_wait(ready, count)
        for step, side in routes:
            if step:
                @pl.when(around(step, side))
                def _():
                    copy(step, side, relay, dates + far_block - step, relay_send).start()

    for step, side in reversed(routes):
        @pl.when(there(-side))
        def _():
            copy(step, side, mine, me, send).wait_recv()

    keep.wait()

    for step, side in routes:
        @pl.when(straight(step, side))
        def _():
            copy(step, side, mine, me - step, send).wait_send()

        if step:
            @pl.when(around(step, side))
            def _():
                copy(step, side, relay, dates + far_block - step, relay_send).wait_send()

    for step, side in late:
        @pl.when(to_first(step, side))
        def _():
            copy(step, side, relay, 0, late_send).wait_send()

    @pl.when(starts | (is_near & (near_block < SHIFTS - 1)))
    def _():
        to_relay(mine, me).wait_send()


def exchange(acquired, dates, tiles):
    shape = acquired.shape
    parts, block, height, breadth = shape
    edge = (SHIFTS, parts, block, EDGE, breadth)
    return pl.pallas_call(
        functools.partial(exchange_kernel, dates, tiles),
        out_shape=(
            jax.ShapeDtypeStruct(shape, jnp.float32),
            jax.ShapeDtypeStruct((SHIFTS - 1,) + shape, jnp.float32),
            jax.ShapeDtypeStruct(edge, jnp.float32),
            jax.ShapeDtypeStruct(edge, jnp.float32),
        ),
        in_specs=[pl.BlockSpec(memory_space=pltpu.HBM)],
        out_specs=(pl.BlockSpec(memory_space=pltpu.VMEM),) * 4,
        scratch_shapes=[
            pltpu.VMEM(shape, jnp.float32),
            pltpu.SemaphoreType.DMA((SHIFTS, 3)),
            pltpu.SemaphoreType.DMA,
            pltpu.SemaphoreType.DMA((SHIFTS - 1,)),
            pltpu.SemaphoreType.DMA((SHIFTS,)),
            pltpu.SemaphoreType.DMA((SHIFTS,)),
            pltpu.SemaphoreType.DMA((SHIFTS, 3)),
            pltpu.SemaphoreType.DMA,
            pltpu.SemaphoreType.DMA((SHIFTS, 3)),
            pltpu.SemaphoreType.REGULAR,
            pltpu.SemaphoreType.REGULAR,
        ],
        compiler_params=pltpu.CompilerParams(
            collective_id=0, has_side_effects=True, vmem_limit_bytes=8 << 20),
        name="exchange",
    )(pltpu.with_memory_space_constraint(acquired, pltpu.HBM))


def window_sums(rows, height):
    width = 2 * row_reach + 1
    sums = [None] * height
    start = 0
    while start < height:
        size = min(width, height - start)
        last = start + width - 1
        tail = rows[last]
        tails = {last: tail}
        for row in range(last - 1, start - 1, -1):
            tail = tail + rows[row]
            tails[row] = tail
        sums[start] = tails[start]
        head = None
        for row in range(start + 1, start + size):
            new = rows[row + width - 1]
            head = new if head is None else head + new
            sums[row] = tails[row] + head
        start += size
    return sums


def coherence_kernel(
    mine, core, above, below, out, parts, sums, power, scale, staged, done,
):
    block, height = out.shape[2], out.shape[4]
    breadth = out.shape[5]
    rows = height + 2 * row_reach
    left = lax.broadcasted_iota(jnp.int32, (breadth, breadth), 0)
    right = lax.broadcasted_iota(jnp.int32, (breadth, breadth), 1)
    band = (jnp.abs(left - right) <= col_reach).astype(jnp.float32).astype(jnp.bfloat16)
    band = jnp.concatenate([band, band], axis=0)

    def split_box(values):
        high = values.astype(jnp.bfloat16)
        low = (values - high.astype(jnp.float32)).astype(jnp.bfloat16)
        return jnp.dot(jnp.concatenate([high, low], axis=1), band, preferred_element_type=jnp.float32)

    def by_date(ref, part):
        tiles = []
        for date in range(block):
            for at in range(0, height, 8):
                tiles.append(ref[part, pl.ds(at * block + date, 8, stride=block), :])
        return jnp.concatenate(tiles, axis=0)

    for step in range(SHIFTS):
        for part in range(2):
            for row in range(rows):
                if row < row_reach:
                    value = above[step, part, pl.ds(EDGE - row_reach + row, block, stride=EDGE), :]
                elif row < row_reach + height:
                    at = pl.ds(row - row_reach, block, stride=height)
                    value = mine[part, at, :] if step == 0 else core[step - 1, part, at, :]
                else:
                    value = below[step, part, pl.ds(row - row_reach - height, block, stride=EDGE), :]
                parts[step, part, row] = value

    for step in range(SHIFTS):
        squares = [parts[step, 0, row] * parts[step, 0, row] + parts[step, 1, row] * parts[step, 1, row] for row in range(rows)]
        for row, value in enumerate(window_sums(squares, height)):
            power[0, row * block:(row + 1) * block, :] = value
        boxed = split_box(by_date(power, 0))
        scale[step] = lax.rsqrt(boxed).reshape(block, height, breadth)

    def anchor(part, row, date):
        return jnp.broadcast_to(parts[0, part, row, pl.ds(date, 1), :], (block, parts.shape[-1]))

    def cross(step):
        for date in range(block):
            real, imag = [], []
            for row in range(rows):
                first_re, first_im = anchor(0, row, date), anchor(1, row, date)
                second_re, second_im = parts[step, 0, row], parts[step, 1, row]
                real.append(first_re * second_re + first_im * second_im)
                imag.append(first_im * second_re - first_re * second_im)
            for part, values in ((0, real), (1, imag)):
                for row, value in enumerate(window_sums(values, height)):
                    sums[date, part, row * block:(row + 1) * block, :] = value
        for date in range(block):
            weight = scale[0, date][None] * scale[step]
            for part in range(2):
                boxed = split_box(by_date(sums.at[date], part))
                staged[step, part, date] = boxed.reshape(block, height, breadth) * weight

    def copy_out(step):
        return pltpu.make_async_copy(staged.at[step], out.at[:, step], done.at[step])

    @pl.loop(0, SHIFTS)
    def _(step):
        cross(step)
        copy_out(step).start()

    @pl.loop(0, SHIFTS)
    def _(step):
        copy_out(step).wait()


def coherence(mine, core, above, below):
    parts, block, height, breadth = mine.shape
    rows = height + 2 * row_reach
    return pl.pallas_call(
        coherence_kernel,
        out_shape=jax.ShapeDtypeStruct((2, SHIFTS, block, block, height, breadth), jnp.float32),
        in_specs=[pl.BlockSpec(memory_space=pltpu.VMEM)] * 4,
        out_specs=pl.BlockSpec(memory_space=pl.ANY),
        scratch_shapes=[
            pltpu.VMEM((SHIFTS, 2, rows, block, breadth), jnp.float32),
            pltpu.VMEM((block, 2, height * block, breadth), jnp.float32),
            pltpu.VMEM((1, height * block, breadth), jnp.float32),
            pltpu.VMEM((SHIFTS, block, height, breadth), jnp.float32),
            pltpu.VMEM((SHIFTS, 2, block, block, height, breadth), jnp.float32),
            pltpu.SemaphoreType.DMA((SHIFTS,)),
        ],
        compiler_params=pltpu.CompilerParams(vmem_limit_bytes=24 << 20),
        name="coherence",
    )(
        mine.reshape(parts, block * height, breadth),
        core.reshape(SHIFTS - 1, parts, block * height, breadth),
        above.reshape(SHIFTS, parts, block * EDGE, breadth),
        below.reshape(SHIFTS, parts, block * EDGE, breadth),
    )


def solution(mesh):
    def on_device(acquired):
        own, core, above, below = exchange(acquired, mesh.shape["date"], mesh.shape["tile"])
        return coherence(own, core, above, below)

    in_specs = (P(None, "date", ("groups", "tile"), None),)
    out_specs = P(None, None, "date", None, ("groups", "tile"), None)
    return jax.shard_map(
        on_device, mesh=mesh, in_specs=in_specs, out_specs=out_specs, check_vma=False
    )
```

```python
import functools

import jax
import jax.numpy as jnp
from jax import lax
from jax.experimental import pallas as pl
from jax.experimental.pallas import tpu as pltpu
from jax.sharding import PartitionSpec as P

SHIFTS = 4
row_reach = 5
col_reach = 2
EDGE = 8
MESH = pl.DeviceIdType.MESH


def when(*conditions):
    return pl.when(functools.reduce(jnp.logical_and, conditions))


def exchange_kernel(
    dates, tiles, mine, own, core, above, below, relay,
    send, got_own, got_core, got_above, got_below, relay_send, relay_got, late_send, ready, late_ready,
):
    me = lax.axis_index("date")
    tile = lax.axis_index("tile")
    height = mine.shape[2]
    near, far = dates * 5 // 16, dates * 3 // 4
    near_block, far_block = me - near, me - far
    starts = me < SHIFTS
    is_near = (near_block >= 0) & (near_block < SHIFTS)
    is_far = (far_block >= 0) & (far_block < SHIFTS - 1)

    def there(side):
        return (tile + side >= 0) & (tile + side < tiles)

    def is_first(date, at):
        return (date == 0) & (at == 0)

    first = is_first(me, tile)
    routes = [(step, side) for step in range(SHIFTS) for side in (1, -1, 0) if (step, side) != (0, 0)]
    late = [(step, side) for step, side in routes if side < 1]

    def signal(semaphore, date, side=0):
        pl.semaphore_signal(
            semaphore, inc=1, device_id={"date": date, "tile": tile + side}, device_id_type=MESH)

    def piece(step, side, source):
        if side == 0:
            return source, core.at[step - 1], got_core.at[step - 1]
        if side == 1:
            return source.at[:, :, pl.ds(height - EDGE, EDGE), :], above.at[step], got_above.at[step]
        return source.at[:, :, pl.ds(0, EDGE), :], below.at[step], got_below.at[step]

    def copy(step, side, source, date, sems):
        src, dst, got = piece(step, side, source)
        return pltpu.make_async_remote_copy(
            src_ref=src, dst_ref=dst, send_sem=sems.at[step, side + 1], recv_sem=got,
            device_id={"date": date, "tile": tile + side}, device_id_type=MESH,
        )

    def straight(step, side):
        return there(side) & (me >= step) & ~is_first(me - step, tile + side)

    def around(step, side):
        return is_far & (step > far_block) & there(side)

    def to_first(step, side):
        return is_near & (near_block == step) & (tile + side == 0)

    barrier = pltpu.get_barrier_semaphore()
    count = jnp.int32(0)
    for step, side in routes:
        @when(there(side), me + step < dates, ~first)
        def _():
            signal(barrier, me + step, side)

        count += straight(step, side).astype(jnp.int32)
        count += (there(side) & (me + step >= dates)).astype(jnp.int32)

        @pl.when(around(step, side))
        def _():
            signal(barrier, dates + far_block - step, side)

    for step, side in late:
        count += (first & there(-side)).astype(jnp.int32)

        @pl.when(to_first(step, side))
        def _():
            signal(barrier, 0, side)

    from_first = is_first(near_block, tile)
    count += first.astype(jnp.int32)

    @pl.when(from_first)
    def _():
        signal(barrier, 0)

    @when(starts, ~first)
    def _():
        signal(barrier, me + near)

    @when(is_near, near_block < SHIFTS - 1)
    def _():
        signal(barrier, near_block + far)

    count += (is_near & ~from_first).astype(jnp.int32) + is_far.astype(jnp.int32)
    pl.semaphore_wait(barrier, count)

    for step, side in routes:
        @pl.when(straight(step, side))
        def _():
            copy(step, side, mine, me - step, send).start()

    keep = pltpu.make_async_copy(mine, own, got_own)
    keep.start()

    @when(is_near, ~from_first)
    def _():
        signal(ready, near_block)

    @pl.when(is_far)
    def _():
        signal(ready, far_block + near)

    for step, side in routes:
        @when(there(side), me + step >= dates)
        def _():
            signal(ready, me + step - dates + far, side)

    for step, side in late:
        @when(first, there(-side))
        def _():
            signal(late_ready, step + near, -side)

    @pl.when(tile == 0)
    def _():
        above[...] = jnp.zeros_like(above)

    @pl.when(tile == tiles - 1)
    def _():
        below[...] = jnp.zeros_like(below)

    def to_relay(source, date):
        return pltpu.make_async_remote_copy(
            src_ref=source, dst_ref=relay, send_sem=relay_send.at[0, 1], recv_sem=relay_got,
            device_id={"date": date, "tile": tile}, device_id_type=MESH,
        )

    @when(starts, ~first)
    def _():
        pl.semaphore_wait(ready, 1)

    @pl.when(starts)
    def _():
        to_relay(mine, me + near).start()

    @pl.when(is_near | is_far)
    def _():
        to_relay(mine, me).wait_recv()

    for step, side in late:
        @pl.when(to_first(step, side))
        def _():
            pl.semaphore_wait(late_ready, 1)
            copy(step, side, relay, 0, late_send).start()

    @when(is_near, near_block < SHIFTS - 1)
    def _():
        pl.semaphore_wait(ready, 1)
        to_relay(relay, near_block + far).start()

    @pl.when(is_far)
    def _():
        count = jnp.int32(0)
        for step, side in routes:
            count += around(step, side).astype(jnp.int32)
        pl.semaphore_wait(ready, count)
        for step, side in routes:
            if step:
                @pl.when(around(step, side))
                def _():
                    copy(step, side, relay, dates + far_block - step, relay_send).start()

    for step, side in reversed(routes):
        @pl.when(there(-side))
        def _():
            copy(step, side, mine, me, send).wait_recv()

    keep.wait()

    for step, side in routes:
        @pl.when(straight(step, side))
        def _():
            copy(step, side, mine, me - step, send).wait_send()

        if step:
            @pl.when(around(step, side))
            def _():
                copy(step, side, relay, dates + far_block - step, relay_send).wait_send()

    for step, side in late:
        @pl.when(to_first(step, side))
        def _():
            copy(step, side, relay, 0, late_send).wait_send()

    @pl.when(starts | (is_near & (near_block < SHIFTS - 1)))
    def _():
        to_relay(mine, me).wait_send()


def exchange(acquired, dates, tiles):
    shape = acquired.shape
    parts, block, height, breadth = shape
    edge = (SHIFTS, parts, block, EDGE, breadth)
    return pl.pallas_call(
        functools.partial(exchange_kernel, dates, tiles),
        out_shape=(
            jax.ShapeDtypeStruct(shape, jnp.float32),
            jax.ShapeDtypeStruct((SHIFTS - 1,) + shape, jnp.float32),
            jax.ShapeDtypeStruct(edge, jnp.float32),
            jax.ShapeDtypeStruct(edge, jnp.float32),
        ),
        in_specs=[pl.BlockSpec(memory_space=pltpu.HBM)],
        out_specs=(pl.BlockSpec(memory_space=pltpu.VMEM),) * 4,
        scratch_shapes=[
            pltpu.VMEM(shape, jnp.float32),
            pltpu.SemaphoreType.DMA((SHIFTS, 3)),
            pltpu.SemaphoreType.DMA,
            pltpu.SemaphoreType.DMA((SHIFTS - 1,)),
            pltpu.SemaphoreType.DMA((SHIFTS,)),
            pltpu.SemaphoreType.DMA((SHIFTS,)),
            pltpu.SemaphoreType.DMA((SHIFTS, 3)),
            pltpu.SemaphoreType.DMA,
            pltpu.SemaphoreType.DMA((SHIFTS, 3)),
            pltpu.SemaphoreType.REGULAR,
            pltpu.SemaphoreType.REGULAR,
        ],
        compiler_params=pltpu.CompilerParams(
            collective_id=0, has_side_effects=True, vmem_limit_bytes=8 << 20),
        name="exchange",
    )(pltpu.with_memory_space_constraint(acquired, pltpu.HBM))


def window_sums(rows, height):
    width = 2 * row_reach + 1
    sums = [None] * height
    start = 0
    while start < height:
        size = min(width, height - start)
        last = start + width - 1
        tail = rows[last]
        tails = {last: tail}
        for row in range(last - 1, start - 1, -1):
            tail = tail + rows[row]
            tails[row] = tail
        sums[start] = tails[start]
        head = None
        for row in range(start + 1, start + size):
            new = rows[row + width - 1]
            head = new if head is None else head + new
            sums[row] = tails[row] + head
        start += size
    return sums


def coherence_kernel(
    mine, core, above, below, out, parts, sums, power, scale, staged, done,
):
    block, height = out.shape[2], out.shape[4]
    breadth = out.shape[5]
    rows = height + 2 * row_reach
    left = lax.broadcasted_iota(jnp.int32, (breadth, breadth), 0)
    right = lax.broadcasted_iota(jnp.int32, (breadth, breadth), 1)
    band = (jnp.abs(left - right) <= col_reach).astype(jnp.float32).astype(jnp.bfloat16)
    band = jnp.concatenate([band, band], axis=0)

    def split_box(values):
        high = values.astype(jnp.bfloat16)
        low = (values - high.astype(jnp.float32)).astype(jnp.bfloat16)
        return jnp.dot(jnp.concatenate([high, low], axis=1), band, preferred_element_type=jnp.float32)

    def by_date(ref, part):
        tiles = []
        for date in range(block):
            for at in range(0, height, 8):
                tiles.append(ref[part, pl.ds(at * block + date, 8, stride=block), :])
        return jnp.concatenate(tiles, axis=0)

    for step in range(SHIFTS):
        for part in range(2):
            for row in range(rows):
                if row < row_reach:
                    value = above[step, part, pl.ds(EDGE - row_reach + row, block, stride=EDGE), :]
                elif row < row_reach + height:
                    at = pl.ds(row - row_reach, block, stride=height)
                    value = mine[part, at, :] if step == 0 else core[step - 1, part, at, :]
                else:
                    value = below[step, part, pl.ds(row - row_reach - height, block, stride=EDGE), :]
                parts[step, part, row] = value

    for step in range(SHIFTS):
        squares = [parts[step, 0, row] * parts[step, 0, row] + parts[step, 1, row] * parts[step, 1, row] for row in range(rows)]
        for row, value in enumerate(window_sums(squares, height)):
            power[0, row * block:(row + 1) * block, :] = value
        boxed = split_box(by_date(power, 0))
        scale[step] = lax.rsqrt(boxed).reshape(block, height, breadth)

    def anchor(part, row, date):
        return jnp.broadcast_to(parts[0, part, row, pl.ds(date, 1), :], (block, parts.shape[-1]))

    def cross(step):
        for date in range(block):
            real, imag = [], []
            for row in range(rows):
                first_re, first_im = anchor(0, row, date), anchor(1, row, date)
                second_re, second_im = parts[step, 0, row], parts[step, 1, row]
                real.append(first_re * second_re + first_im * second_im)
                imag.append(first_im * second_re - first_re * second_im)
            for part, values in ((0, real), (1, imag)):
                for row, value in enumerate(window_sums(values, height)):
                    sums[date, part, row * block:(row + 1) * block, :] = value
        for date in range(block):
            weight = scale[0, date][None] * scale[step]
            for part in range(2):
                boxed = split_box(by_date(sums.at[date], part))
                staged[step, part, date] = boxed.reshape(block, height, breadth) * weight

    def copy_out(step):
        return pltpu.make_async_copy(staged.at[step], out.at[:, step], done.at[step])

    @pl.loop(0, SHIFTS)
    def _(step):
        cross(step)
        copy_out(step).start()

    @pl.loop(0, SHIFTS)
    def _(step):
        copy_out(step).wait()


def coherence(mine, core, above, below):
    parts, block, height, breadth = mine.shape
    rows = height + 2 * row_reach
    return pl.pallas_call(
        coherence_kernel,
        out_shape=jax.ShapeDtypeStruct((2, SHIFTS, block, block, height, breadth), jnp.float32),
        in_specs=[pl.BlockSpec(memory_space=pltpu.VMEM)] * 4,
        out_specs=pl.BlockSpec(memory_space=pl.ANY),
        scratch_shapes=[
            pltpu.VMEM((SHIFTS, 2, rows, block, breadth), jnp.float32),
            pltpu.VMEM((block, 2, height * block, breadth), jnp.float32),
            pltpu.VMEM((1, height * block, breadth), jnp.float32),
            pltpu.VMEM((SHIFTS, block, height, breadth), jnp.float32),
            pltpu.VMEM((SHIFTS, 2, block, block, height, breadth), jnp.float32),
            pltpu.SemaphoreType.DMA((SHIFTS,)),
        ],
        compiler_params=pltpu.CompilerParams(vmem_limit_bytes=24 << 20),
        name="coherence",
    )(
        mine.reshape(parts, block * height, breadth),
        core.reshape(SHIFTS - 1, parts, block * height, breadth),
        above.reshape(SHIFTS, parts, block * EDGE, breadth),
        below.reshape(SHIFTS, parts, block * EDGE, breadth),
    )


def solution(mesh):
    def on_device(acquired):
        own, core, above, below = exchange(acquired, mesh.shape["date"], mesh.shape["tile"])
        return coherence(own, core, above, below)

    in_specs = (P(None, "date", ("groups", "tile"), None),)
    out_specs = P(None, None, "date", None, ("groups", "tile"), None)
    return jax.shard_map(
        on_device, mesh=mesh, in_specs=in_specs, out_specs=out_specs, check_vma=False
    )
```

```python
import functools

import jax
import jax.numpy as jnp
from jax import lax
from jax.experimental import pallas as pl
from jax.experimental.pallas import tpu as pltpu
from jax.sharding import PartitionSpec as P

SHIFTS = 4
row_reach = 5
col_reach = 2
EDGE = 8
MESH = pl.DeviceIdType.MESH


def when(*conditions):
    return pl.when(functools.reduce(jnp.logical_and, conditions))


def exchange_kernel(
    dates, tiles, mine, above, rows, boxed, partial, partial_power, scale, own, core, below, relay, sums,
    send, got_own, got_core, got_above, got_below, relay_send, relay_got, late_send, ready, late_ready,
):
    me = lax.axis_index("date")
    tile = lax.axis_index("tile")
    block, height, breadth = mine.shape[1:]
    near, far = dates * 5 // 16, dates * 3 // 4
    near_block, far_block = me - near, me - far
    starts = me < SHIFTS
    is_near = (near_block >= 0) & (near_block < SHIFTS)
    is_far = (far_block >= 0) & (far_block < SHIFTS - 1)

    def there(side):
        return (tile + side >= 0) & (tile + side < tiles)

    def is_first(date, at):
        return (lax.axis_index("groups") == 0) & (date == 0) & (at == 0)

    first = is_first(me, tile)
    routes = [(step, side) for step in range(SHIFTS) for side in (1, -1, 0) if (step, side) != (0, 0)]
    late = [(step, side) for step, side in routes if side < 1]

    def signal(semaphore, date, side=0):
        pl.semaphore_signal(
            semaphore, inc=1, device_id={"date": date, "tile": tile + side}, device_id_type=MESH)

    def piece(step, side, source):
        if side == 0:
            return source, core.at[step - 1], got_core.at[step - 1]
        if side == 1:
            return source.at[:, :, pl.ds(height - EDGE, EDGE), :], above.at[step], got_above.at[step]
        return source.at[:, :, pl.ds(0, EDGE), :], below.at[step], got_below.at[step]

    def copy(step, side, source, date, sems):
        src, dst, got = piece(step, side, source)
        return pltpu.make_async_remote_copy(
            src_ref=src, dst_ref=dst, send_sem=sems.at[step, side + 1], recv_sem=got,
            device_id={"date": date, "tile": tile + side}, device_id_type=MESH,
        )

    def straight(step, side):
        return there(side) & (me >= step) & ~is_first(me - step, tile + side)

    def around(step, side):
        return is_far & (step > far_block) & there(side)

    def to_first(step, side):
        return is_near & (near_block == step) & is_first(0, tile + side)

    barrier = pltpu.get_barrier_semaphore()
    count = jnp.int32(0)
    for step, side in routes:
        @when(there(side), me + step < dates, ~first)
        def _():
            signal(barrier, me + step, side)

        count += straight(step, side).astype(jnp.int32)
        count += (there(side) & (me + step >= dates)).astype(jnp.int32)

        @pl.when(around(step, side))
        def _():
            signal(barrier, dates + far_block - step, side)

    for step, side in late:
        count += (first & there(-side)).astype(jnp.int32)

        @pl.when(to_first(step, side))
        def _():
            signal(barrier, 0, side)

    from_first = is_first(near_block, tile)
    count += first.astype(jnp.int32)

    @pl.when(from_first)
    def _():
        signal(barrier, 0)

    @when(starts, ~first)
    def _():
        signal(barrier, me + near)

    @when(is_near, near_block < SHIFTS - 1)
    def _():
        signal(barrier, near_block + far)

    count += (is_near & ~from_first).astype(jnp.int32) + is_far.astype(jnp.int32)
    pl.semaphore_wait(barrier, count)

    for step, side in routes:
        @pl.when(straight(step, side))
        def _():
            copy(step, side, mine, me - step, send).start()

    keep = pltpu.make_async_copy(mine, own, got_own)
    keep.start()

    @when(is_near, ~from_first)
    def _():
        signal(ready, near_block)

    @pl.when(is_far)
    def _():
        signal(ready, far_block + near)

    for step, side in routes:
        @when(there(side), me + step >= dates)
        def _():
            signal(ready, me + step - dates + far, side)

    for step, side in late:
        @when(first, there(-side))
        def _():
            signal(late_ready, step + near, -side)

    @pl.when(tile == 0)
    def _():
        above[...] = jnp.zeros_like(above)

    @pl.when(tile == tiles - 1)
    def _():
        below[...] = jnp.zeros_like(below)

    def to_relay(source, date):
        return pltpu.make_async_remote_copy(
            src_ref=source, dst_ref=relay, send_sem=relay_send.at[0, 1], recv_sem=relay_got,
            device_id={"date": date, "tile": tile}, device_id_type=MESH,
        )

    @pl.when(first)
    def _():
        to_relay(mine, near).start()

    @pl.when(is_far)
    def _():
        to_relay(mine, me).wait_recv()
        count = jnp.int32(0)
        for step, side in routes:
            count += around(step, side).astype(jnp.int32)
        pl.semaphore_wait(ready, count)
        for step, side in routes:
            if step:
                @pl.when(around(step, side))
                def _():
                    copy(step, side, relay, dates + far_block - step, relay_send).start()

    for step, side in reversed(routes):
        if (step, side) != (0, 1):
            @pl.when(there(-side))
            def _():
                copy(step, side, mine, me, send).wait_recv()

    keep.wait()

    band = band_table(breadth)
    total = height + 2 * row_reach
    above_rows = above.reshape(SHIFTS, 2, block * EDGE, breadth)
    below_rows = below.reshape(SHIFTS, 2, block * EDGE, breadth)
    own_rows = own.reshape(2, block * height, breadth)
    core_rows = core.reshape(SHIFTS - 1, 2, block * height, breadth)

    for step in range(SHIFTS):
        for part in range(2):
            for row in range(row_reach):
                rows[step, part, row_reach + height + row] = below_rows[step, part, pl.ds(row, block, stride=EDGE), :]
                if step:
                    at = pl.ds(EDGE - row_reach + row, block, stride=EDGE)
                    rows[step, part, row] = above_rows[step, part, at, :]

    for row in range(height):
        for part in range(2):
            at = pl.ds(row, block, stride=height)
            rows[0, part, row_reach + row] = own_rows[part, at, :]
            for step in range(1, SHIFTS):
                rows[step, part, row_reach + row] = core_rows[step - 1, part, at, :]

    def store(values, ref):
        for row, value in enumerate(values):
            ref[row * block:(row + 1) * block, :] = value

    for step in range(SHIFTS):
        squares = {row: square(rows, step, row) for row in range(row_reach if step == 0 else 0, total)}
        if step == 0:
            store(inner_sums(squares, EDGE), partial_power)
        else:
            store(window_sums(squares, 0, EDGE), sums.at[0])
            scale[step, 0] = lax.rsqrt(box_columns(by_date(sums.at[0], block), band)).reshape(block, EDGE, breadth)
        store(window_sums(squares, EDGE, height), sums.at[1])
        scale[step, 1] = lax.rsqrt(box_columns(by_date(sums.at[1], block), band)).reshape(block, EDGE, breadth)

    @pl.loop(0, SHIFTS)
    def _(step):
        for date in range(block):
            real, imag = products(rows, rows, step, date, range(row_reach, total))
            for part, values in enumerate((real, imag)):
                store(inner_sums(values, EDGE), partial.at[step, date, part])
                store(window_sums(values, EDGE, height), sums.at[date * 2 + part])
        for date in range(block):
            weight = scale[0, 1, date][None] * scale[step, 1]
            for part in range(2):
                columns = box_columns(by_date(sums.at[date * 2 + part], block), band)
                boxed[part, step, date] = columns.reshape(block, EDGE, breadth) * weight

    @when(starts, ~first)
    def _():
        pl.semaphore_wait(ready, 1)
        to_relay(mine, me + near).start()

    for step, side in late:
        @pl.when(to_first(step, side))
        def _():
            to_relay(mine, me).wait_recv()
            pl.semaphore_wait(late_ready, 1)
            copy(step, side, relay, 0, late_send).start()

    serves_first = functools.reduce(jnp.logical_or, [to_first(step, side) for step, side in late])

    @when(is_near, ~serves_first)
    def _():
        to_relay(mine, me).wait_recv()

    @when(is_near, near_block < SHIFTS - 1)
    def _():
        pl.semaphore_wait(ready, 1)
        to_relay(relay, near_block + far).start()

    @pl.when(there(-1))
    def _():
        copy(0, 1, mine, me, send).wait_recv()

    for step, side in routes:
        @pl.when(straight(step, side))
        def _():
            copy(step, side, mine, me - step, send).wait_send()

        if step:
            @pl.when(around(step, side))
            def _():
                copy(step, side, relay, dates + far_block - step, relay_send).wait_send()

    for step, side in late:
        @pl.when(to_first(step, side))
        def _():
            copy(step, side, relay, 0, late_send).wait_send()

    @pl.when(starts | (is_near & (near_block < SHIFTS - 1)))
    def _():
        to_relay(mine, me).wait_send()


def exchange(acquired, dates, tiles):
    parts, block, height, breadth = acquired.shape
    total = height + 2 * row_reach
    edge = (SHIFTS, parts, block, EDGE, breadth)
    results = (
        edge,
        (SHIFTS, parts, total, block, breadth),
        (2, SHIFTS, block, block, EDGE, breadth),
        (SHIFTS, block, 2, EDGE * block, breadth),
        (EDGE * block, breadth),
        (SHIFTS, 2, block, EDGE, breadth),
    )
    return pl.pallas_call(
        functools.partial(exchange_kernel, dates, tiles),
        out_shape=tuple(jax.ShapeDtypeStruct(shape, jnp.float32) for shape in results),
        in_specs=[pl.BlockSpec(memory_space=pltpu.HBM)],
        out_specs=(pl.BlockSpec(memory_space=pltpu.VMEM),) * len(results),
        scratch_shapes=[
            pltpu.VMEM(acquired.shape, jnp.float32),
            pltpu.VMEM((SHIFTS - 1,) + acquired.shape, jnp.float32),
            pltpu.VMEM(edge, jnp.float32),
            pltpu.VMEM(acquired.shape, jnp.float32),
            pltpu.VMEM((2 * block, EDGE * block, breadth), jnp.float32),
            pltpu.SemaphoreType.DMA((SHIFTS, 3)),
            pltpu.SemaphoreType.DMA,
            pltpu.SemaphoreType.DMA((SHIFTS - 1,)),
            pltpu.SemaphoreType.DMA((SHIFTS,)),
            pltpu.SemaphoreType.DMA((SHIFTS,)),
            pltpu.SemaphoreType.DMA((SHIFTS, 3)),
            pltpu.SemaphoreType.DMA,
            pltpu.SemaphoreType.DMA((SHIFTS, 3)),
            pltpu.SemaphoreType.REGULAR,
            pltpu.SemaphoreType.REGULAR,
        ],
        compiler_params=pltpu.CompilerParams(
            collective_id=0, has_side_effects=True, vmem_limit_bytes=16 << 20),
        name="exchange",
    )(pltpu.with_memory_space_constraint(acquired, pltpu.HBM))


def band_table(breadth):
    left = lax.broadcasted_iota(jnp.int32, (breadth, breadth), 0)
    right = lax.broadcasted_iota(jnp.int32, (breadth, breadth), 1)
    band = (jnp.abs(left - right) <= col_reach).astype(jnp.float32).astype(jnp.bfloat16)
    return jnp.concatenate([band, band], axis=0)


def box_columns(values, band):
    high = values.astype(jnp.bfloat16)
    low = (values - high.astype(jnp.float32)).astype(jnp.bfloat16)
    return jnp.dot(jnp.concatenate([high, low], axis=1), band, preferred_element_type=jnp.float32)


def by_date(ref, block):
    return jnp.concatenate([ref[pl.ds(date, EDGE, stride=block), :] for date in range(block)], axis=0)


def square(rows, step, row):
    real, imag = rows[step, 0, row], rows[step, 1, row]
    return real * real + imag * imag


def products(first, second, step, date, which):
    real, imag = {}, {}
    for row in which:
        second_re, second_im = second[step, 0, row], second[step, 1, row]
        first_re = jnp.broadcast_to(first[0, 0, row, pl.ds(date, 1), :], second_re.shape)
        first_im = jnp.broadcast_to(first[0, 1, row, pl.ds(date, 1), :], second_re.shape)
        real[row] = first_re * second_re + first_im * second_im
        imag[row] = first_im * second_re - first_re * second_im
    return real, imag


def window_sums(rows, start, stop):
    last = start + 2 * row_reach
    tails = {last: rows[last]}
    for row in range(last - 1, start - 1, -1):
        tails[row] = tails[row + 1] + rows[row]
    sums, head = [tails[start]], None
    for row in range(start + 1, stop):
        new = rows[row + 2 * row_reach]
        head = new if head is None else head + new
        sums.append(tails[row] + head)
    return sums


def inner_sums(rows, count):
    last = 2 * row_reach
    tails = {last: rows[last]}
    for row in range(last - 1, row_reach - 1, -1):
        tails[row] = tails[row + 1] + rows[row]
    sums, head = [tails[row_reach]], None
    for row in range(1, count):
        new = rows[row + last]
        head = new if head is None else head + new
        sums.append(tails[max(row, row_reach)] + head)
    return sums


def coherence_kernel(
    above, rows, boxed, partial, partial_power, scale, out, top, sums, weights, staged, done, done_boxed,
):
    block, breadth = out.shape[2], out.shape[5]
    finished = pltpu.make_async_copy(boxed, out.at[:, :, :, :, pl.ds(EDGE, EDGE), :], done_boxed)
    finished.start()
    band = band_table(breadth)
    which = range(row_reach)
    above = above.reshape(SHIFTS, 2, block * EDGE, breadth)

    for part in range(2):
        for row in which:
            top[0, part, row] = above[0, part, pl.ds(EDGE - row_reach + row, block, stride=EDGE), :]
            for step in range(1, SHIFTS):
                top[step, part, row] = rows[step, part, row]

    def add_top(values, inner, ref):
        tail = None
        for row in reversed(which):
            tail = values[row] if tail is None else tail + values[row]
            at = pl.ds(row * block, block)
            ref[at, :] = inner[at, :] + tail
        at = pl.ds(row_reach * block, (EDGE - row_reach) * block)
        ref[at, :] = inner[at, :]

    add_top({row: square(top, 0, row) for row in which}, partial_power, sums.at[0])
    weights[0] = lax.rsqrt(box_columns(by_date(sums.at[0], block), band)).reshape(block, EDGE, breadth)
    for step in range(1, SHIFTS):
        weights[step] = scale[step, 0]

    def copy_out(step):
        return pltpu.make_async_copy(
            staged.at[step], out.at[:, step, :, :, pl.ds(0, EDGE), :], done.at[step])

    @pl.loop(0, SHIFTS)
    def _(step):
        for date in range(block):
            both = products(top, top, step, date, which)
            for part, values in enumerate(both):
                add_top(values, partial.at[step, date, part], sums.at[date * 2 + part])
        for date in range(block):
            weight = weights[0, date][None] * weights[step]
            for part in range(2):
                columns = box_columns(by_date(sums.at[date * 2 + part], block), band)
                staged[step, part, date] = columns.reshape(block, EDGE, breadth) * weight
        copy_out(step).start()

    @pl.loop(0, SHIFTS)
    def _(step):
        copy_out(step).wait()

    finished.wait()


def coherence(block, height, breadth, *values):
    return pl.pallas_call(
        coherence_kernel,
        out_shape=jax.ShapeDtypeStruct((2, SHIFTS, block, block, height, breadth), jnp.float32),
        in_specs=[pl.BlockSpec(memory_space=pltpu.VMEM)] * len(values),
        out_specs=pl.BlockSpec(memory_space=pl.ANY),
        scratch_shapes=[
            pltpu.VMEM((SHIFTS, 2, row_reach, block, breadth), jnp.float32),
            pltpu.VMEM((2 * block, EDGE * block, breadth), jnp.float32),
            pltpu.VMEM((SHIFTS, block, EDGE, breadth), jnp.float32),
            pltpu.VMEM((SHIFTS, 2, block, block, EDGE, breadth), jnp.float32),
            pltpu.SemaphoreType.DMA((SHIFTS,)),
            pltpu.SemaphoreType.DMA,
        ],
        compiler_params=pltpu.CompilerParams(vmem_limit_bytes=16 << 20),
        name="coherence",
    )(*values)


def solution(mesh):
    def on_device(acquired):
        return coherence(*acquired.shape[1:], *exchange(acquired, mesh.shape["date"], mesh.shape["tile"]))

    in_specs = (P(None, "date", ("groups", "tile"), None),)
    out_specs = P(None, None, "date", None, ("groups", "tile"), None)
    return jax.shard_map(
        on_device, mesh=mesh, in_specs=in_specs, out_specs=out_specs, check_vma=False
    )
```

```python
import functools

import jax
import jax.numpy as jnp
from jax import lax
from jax.experimental import pallas as pl
from jax.experimental.pallas import tpu as pltpu
from jax.sharding import PartitionSpec as P

SHIFTS = 4
row_reach = 5
col_reach = 2
EDGE = 8
MESH = pl.DeviceIdType.MESH


def when(*conditions):
    return pl.when(functools.reduce(jnp.logical_and, conditions))


def exchange_kernel(
    dates, tiles, mine, boxed, staged, above, rows, partial, partial_power, weights, band_out, own, core, below, relay, sums, scale,
    send, got_own, got_core, got_above, got_below, relay_send, relay_got, late_send, ready, late_ready,
):
    me = lax.axis_index("date")
    tile = lax.axis_index("tile")
    block, height, breadth = mine.shape[1:]
    near, far = dates * 5 // 16, dates * 3 // 4
    near_block, far_block = me - near, me - far
    starts = me < SHIFTS
    is_near = (near_block >= 0) & (near_block < SHIFTS)
    is_far = (far_block >= 0) & (far_block < SHIFTS - 1)

    def there(side):
        return (tile + side >= 0) & (tile + side < tiles)

    def is_first(date, at):
        return (lax.axis_index("groups") == 0) & (date == 0) & (at == 0)

    first = is_first(me, tile)
    routes = [(step, side) for step in range(SHIFTS) for side in (1, -1, 0) if (step, side) != (0, 0)]
    late = [(step, side) for step, side in routes if side < 1]

    def signal(semaphore, date, side=0):
        pl.semaphore_signal(
            semaphore, inc=1, device_id={"date": date, "tile": tile + side}, device_id_type=MESH)

    def piece(step, side, source):
        if side == 0:
            return source, core.at[step - 1], got_core.at[step - 1]
        if side == 1:
            return source.at[:, :, pl.ds(height - EDGE, EDGE), :], above.at[step], got_above.at[step]
        return source.at[:, :, pl.ds(0, EDGE), :], below.at[step], got_below.at[step]

    def copy(step, side, source, date, sems):
        src, dst, got = piece(step, side, source)
        return pltpu.make_async_remote_copy(
            src_ref=src, dst_ref=dst, send_sem=sems.at[step, side + 1], recv_sem=got,
            device_id={"date": date, "tile": tile + side}, device_id_type=MESH,
        )

    def straight(step, side):
        return there(side) & (me >= step) & ~is_first(me - step, tile + side)

    def around(step, side):
        return is_far & (step > far_block) & there(side)

    def to_first(step, side):
        return is_near & (near_block == step) & is_first(0, tile + side)

    barrier = pltpu.get_barrier_semaphore()
    from_first = is_first(near_block, tile)

    @pl.when(~first)
    def _():
        for step, side in routes:
            @when(there(side), me + step < dates)
            def _():
                signal(barrier, me + step, side)

            @pl.when(around(step, side))
            def _():
                signal(barrier, dates + far_block - step, side)

        for step, side in late:
            @pl.when(to_first(step, side))
            def _():
                signal(barrier, 0, side)

        @pl.when(from_first)
        def _():
            signal(barrier, 0)

        @pl.when(starts)
        def _():
            signal(barrier, me + near)

        @when(is_near, near_block < SHIFTS - 1)
        def _():
            signal(barrier, near_block + far)

    count = first.astype(jnp.int32) + (is_near & ~from_first).astype(jnp.int32) + is_far.astype(jnp.int32)
    for step, side in routes:
        count += straight(step, side).astype(jnp.int32)
        count += (there(side) & (me + step >= dates)).astype(jnp.int32)
    for step, side in late:
        count += (first & there(-side)).astype(jnp.int32)
    pl.semaphore_wait(barrier, count)

    for step, side in routes:
        @pl.when(straight(step, side))
        def _():
            copy(step, side, mine, me - step, send).start()

    keep = pltpu.make_async_copy(mine, own, got_own)
    keep.start()

    @when(is_near, ~from_first)
    def _():
        signal(ready, near_block)

    @pl.when(is_far)
    def _():
        signal(ready, far_block + near)

    for step, side in routes:
        @when(there(side), me + step >= dates)
        def _():
            signal(ready, me + step - dates + far, side)

    for step, side in late:
        @when(first, there(-side))
        def _():
            signal(late_ready, step + near, -side)

    @pl.when(tile == 0)
    def _():
        above[...] = jnp.zeros_like(above)

    @pl.when(tile == tiles - 1)
    def _():
        below[...] = jnp.zeros_like(below)

    def to_relay(source, date):
        return pltpu.make_async_remote_copy(
            src_ref=source, dst_ref=relay, send_sem=relay_send.at[0, 1], recv_sem=relay_got,
            device_id={"date": date, "tile": tile}, device_id_type=MESH,
        )

    @pl.when(first)
    def _():
        to_relay(mine, near).start()

    @pl.when(is_far)
    def _():
        to_relay(mine, me).wait_recv()
        count = jnp.int32(0)
        for step, side in routes:
            count += around(step, side).astype(jnp.int32)
        pl.semaphore_wait(ready, count)
        for step, side in routes:
            if step:
                @pl.when(around(step, side))
                def _():
                    copy(step, side, relay, dates + far_block - step, relay_send).start()

    for step, side in reversed(routes):
        if (step, side) != (0, 1):
            @pl.when(there(-side))
            def _():
                copy(step, side, mine, me, send).wait_recv()

    keep.wait()

    band = band_table(breadth)
    band_out[...] = band
    total = height + 2 * row_reach
    above_rows = above.reshape(SHIFTS, 2, block * EDGE, breadth)
    below_rows = below.reshape(SHIFTS, 2, block * EDGE, breadth)
    own_rows = own.reshape(2, block * height, breadth)
    core_rows = core.reshape(SHIFTS - 1, 2, block * height, breadth)

    for step in range(SHIFTS):
        for part in range(2):
            for row in range(row_reach):
                rows[step, part, row_reach + height + row] = below_rows[step, part, pl.ds(row, block, stride=EDGE), :]
                if step:
                    at = pl.ds(EDGE - row_reach + row, block, stride=EDGE)
                    rows[step, part, row] = above_rows[step, part, at, :]

    for row in range(height):
        for part in range(2):
            at = pl.ds(row, block, stride=height)
            rows[0, part, row_reach + row] = own_rows[part, at, :]
            for step in range(1, SHIFTS):
                rows[step, part, row_reach + row] = core_rows[step - 1, part, at, :]

    def store(values, ref):
        for row, value in enumerate(values):
            ref[row * block:(row + 1) * block, :] = value

    for step in range(SHIFTS):
        squares = {row: square(rows, step, row) for row in range(row_reach if step == 0 else 0, total)}
        upper = inner_sums(squares, EDGE) if step == 0 else window_sums(squares, 0, EDGE)
        upper = jnp.concatenate(upper, axis=0)
        if step == 0:
            partial_power[...] = upper
        weights[step] = lax.rsqrt(box_columns(upper, band))
        store(window_sums(squares, EDGE, height), sums.at[0])
        scale[step] = lax.rsqrt(box_columns(by_date(sums.at[0], block), band)).reshape(block, EDGE, breadth)

    inner = slice(row_reach * block, EDGE * block)
    staged_rows = staged.reshape(SHIFTS, 2, block, block * EDGE, breadth)

    @pl.loop(0, SHIFTS)
    def _(step):
        upper = []
        for date in range(block):
            real, imag = products(rows, rows, step, date, range(row_reach, total))
            for part, values in enumerate((real, imag)):
                found = inner_sums(values, EDGE)
                store(found[:row_reach], partial.at[step, date, part])
                upper += found[row_reach:]
                store(window_sums(values, EDGE, height), sums.at[date * 2 + part])
        columns = box_columns(jnp.concatenate(upper, axis=0), band)
        for date in range(block):
            for row in range(row_reach, EDGE):
                weight = date_weight(weights, weights.at[step], row, date, block)
                for part in range(2):
                    at = ((date * 2 + part) * (EDGE - row_reach) + row - row_reach) * block
                    staged_rows[step, part, date, pl.ds(row, block, stride=EDGE), :] = columns[at:at + block] * weight
        for date in range(block):
            weight = scale[0, date][None] * scale[step]
            for part in range(2):
                columns = box_columns(by_date(sums.at[date * 2 + part], block), band)
                boxed[step, part, date] = columns.reshape(block, EDGE, breadth) * weight

    @when(starts, ~first)
    def _():
        pl.semaphore_wait(ready, 1)
        to_relay(mine, me + near).start()

    for step, side in late:
        @pl.when(to_first(step, side))
        def _():
            to_relay(mine, me).wait_recv()
            pl.semaphore_wait(late_ready, 1)
            copy(step, side, relay, 0, late_send).start()

    serves_first = functools.reduce(jnp.logical_or, [to_first(step, side) for step, side in late])

    @when(is_near, ~serves_first)
    def _():
        to_relay(mine, me).wait_recv()

    @when(is_near, near_block < SHIFTS - 1)
    def _():
        pl.semaphore_wait(ready, 1)
        to_relay(relay, near_block + far).start()

    for step, side in routes:
        @pl.when(straight(step, side))
        def _():
            copy(step, side, mine, me - step, send).wait_send()

        if step:
            @pl.when(around(step, side))
            def _():
                copy(step, side, relay, dates + far_block - step, relay_send).wait_send()

    for step, side in late:
        @pl.when(to_first(step, side))
        def _():
            copy(step, side, relay, 0, late_send).wait_send()

    @pl.when(starts | (is_near & (near_block < SHIFTS - 1)))
    def _():
        to_relay(mine, me).wait_send()

    @pl.when(there(-1))
    def _():
        copy(0, 1, mine, me, send).wait_recv()


def exchange(acquired, dates, tiles):
    parts, block, height, breadth = acquired.shape
    total = height + 2 * row_reach
    edge = (SHIFTS, parts, block, EDGE, breadth)
    tile = (SHIFTS, 2, block, block, EDGE, breadth)
    results = (
        tile,
        tile,
        edge,
        (SHIFTS, parts, total, block, breadth),
        (SHIFTS, block, 2, row_reach * block, breadth),
        (EDGE * block, breadth),
        (SHIFTS, EDGE * block, breadth),
    )
    return pl.pallas_call(
        functools.partial(exchange_kernel, dates, tiles),
        out_shape=tuple(jax.ShapeDtypeStruct(shape, jnp.float32) for shape in results) + (
            jax.ShapeDtypeStruct((2 * breadth, breadth), jnp.bfloat16),),
        in_specs=[pl.BlockSpec(memory_space=pltpu.HBM)],
        out_specs=(pl.BlockSpec(memory_space=pltpu.VMEM),) * (len(results) + 1),
        scratch_shapes=[
            pltpu.VMEM(acquired.shape, jnp.float32),
            pltpu.VMEM((SHIFTS - 1,) + acquired.shape, jnp.float32),
            pltpu.VMEM(edge, jnp.float32),
            pltpu.VMEM(acquired.shape, jnp.float32),
            pltpu.VMEM((2 * block, EDGE * block, breadth), jnp.float32),
            pltpu.VMEM((SHIFTS, block, EDGE, breadth), jnp.float32),
            pltpu.SemaphoreType.DMA((SHIFTS, 3)),
            pltpu.SemaphoreType.DMA,
            pltpu.SemaphoreType.DMA((SHIFTS - 1,)),
            pltpu.SemaphoreType.DMA((SHIFTS,)),
            pltpu.SemaphoreType.DMA((SHIFTS,)),
            pltpu.SemaphoreType.DMA((SHIFTS, 3)),
            pltpu.SemaphoreType.DMA,
            pltpu.SemaphoreType.DMA((SHIFTS, 3)),
            pltpu.SemaphoreType.REGULAR,
            pltpu.SemaphoreType.REGULAR,
        ],
        compiler_params=pltpu.CompilerParams(
            collective_id=0, has_side_effects=True, vmem_limit_bytes=16 << 20),
        name="exchange",
    )(pltpu.with_memory_space_constraint(acquired, pltpu.HBM))


def band_table(breadth):
    left = lax.broadcasted_iota(jnp.int32, (breadth, breadth), 0)
    right = lax.broadcasted_iota(jnp.int32, (breadth, breadth), 1)
    band = (jnp.abs(left - right) <= col_reach).astype(jnp.float32).astype(jnp.bfloat16)
    return jnp.concatenate([band, band], axis=0)


def box_columns(values, band):
    high = values.astype(jnp.bfloat16)
    low = (values - high.astype(jnp.float32)).astype(jnp.bfloat16)
    return jnp.dot(jnp.concatenate([high, low], axis=1), band, preferred_element_type=jnp.float32)


def by_date(ref, block):
    return jnp.concatenate([ref[pl.ds(date, EDGE, stride=block), :] for date in range(block)], axis=0)


def square(rows, step, row):
    real, imag = rows[step, 0, row], rows[step, 1, row]
    return real * real + imag * imag


def products(first, second, step, date, which):
    real, imag = {}, {}
    for row in which:
        second_re, second_im = second[step, 0, row], second[step, 1, row]
        first_re = jnp.broadcast_to(first[0, 0, row, pl.ds(date, 1), :], second_re.shape)
        first_im = jnp.broadcast_to(first[0, 1, row, pl.ds(date, 1), :], second_re.shape)
        real[row] = first_re * second_re + first_im * second_im
        imag[row] = first_im * second_re - first_re * second_im
    return real, imag


def window_sums(rows, start, stop):
    last = start + 2 * row_reach
    tails = {last: rows[last]}
    for row in range(last - 1, start - 1, -1):
        tails[row] = tails[row + 1] + rows[row]
    sums, head = [tails[start]], None
    for row in range(start + 1, stop):
        new = rows[row + 2 * row_reach]
        head = new if head is None else head + new
        sums.append(tails[row] + head)
    return sums


def inner_sums(rows, count):
    last = 2 * row_reach
    tails = {last: rows[last]}
    for row in range(last - 1, row_reach - 1, -1):
        tails[row] = tails[row + 1] + rows[row]
    sums, head = [tails[row_reach]], None
    for row in range(1, count):
        new = rows[row + last]
        head = new if head is None else head + new
        sums.append(tails[max(row, row_reach)] + head)
    return sums


def date_weight(first, second, row, date, block):
    return jnp.broadcast_to(first[0, pl.ds(row * block + date, 1), :], (block, second.shape[-1])) * second[pl.ds(row * block, block), :]


def coherence_kernel(
    boxed, staged_before, above, rows, partial, partial_power, weights, band, out, staged, top, found, done, done_boxed,
):
    block, height, breadth = out.shape[3:]

    def copy_boxed(step):
        return pltpu.make_async_copy(
            boxed.at[step], out.at[:, step, :, :, pl.ds(EDGE, height - EDGE), :], done_boxed.at[step])

    for step in range(SHIFTS):
        copy_boxed(step).start()
    which = range(row_reach)
    above = above.reshape(SHIFTS, 2, block * EDGE, breadth)
    staged_rows = staged.reshape(SHIFTS, 2, block, block * EDGE, breadth)

    for part in range(2):
        for row in which:
            top[0, part, row] = above[0, part, pl.ds(EDGE - row_reach + row, block, stride=EDGE), :]

    def with_top(values, inner):
        tails = [values[row_reach - 1]]
        for row in reversed(which[:-1]):
            tails.insert(0, tails[0] + values[row])
        return [tails[row] + inner[row * block:(row + 1) * block, :] for row in which]

    power = with_top({row: square(top, 0, row) for row in which}, partial_power)
    power = box_columns(jnp.concatenate(power, axis=0), band[...])
    size = block // 2

    def copy_out(step, half):
        dates = pl.ds(half * size, size)
        return pltpu.make_async_copy(
            staged.at[step, :, dates], out.at[:, step, dates, :, pl.ds(0, EDGE), :], done.at[step, half])

    def begin(step, half):
        upper = []
        for date in range(half * size, (half + 1) * size):
            both = products(top, rows if step else top, step, date, which)
            for part, values in enumerate(both):
                upper += with_top(values, partial.at[step, date, part])
        return box_columns(jnp.concatenate(upper, axis=0), band[...])

    def end(step, half, columns):
        for date in range(size):
            for row in which:
                weight = date_weight(found, weights.at[step] if step else found.at[0], row, half * size + date, block)
                for part in range(2):
                    at = ((date * 2 + part) * row_reach + row) * block
                    rows_of = pl.ds(row, block, stride=EDGE)
                    staged_rows[step, part, half * size + date, rows_of, :] = columns[at:at + block] * weight
        copy_out(step, half).start()

    pieces = [(step, half) for step in range(SHIFTS) for half in range(2)]
    begun = None
    for piece in pieces:
        columns = begin(*piece)
        if begun is None:
            found[0] = lax.rsqrt(power)
        else:
            end(*begun)
        begun = (*piece, columns)
    end(*begun)

    for step in range(SHIFTS):
        copy_boxed(step).wait()
    for piece in pieces:
        copy_out(*piece).wait()


def coherence(height, boxed, staged, *values):
    block, breadth = staged.shape[2], staged.shape[5]
    vmem = pl.BlockSpec(memory_space=pltpu.VMEM)
    return pl.pallas_call(
        coherence_kernel,
        out_shape=(
            pltpu.HBM((2, SHIFTS, block, block, height, breadth), jnp.float32),
            jax.ShapeDtypeStruct(staged.shape, jnp.float32),
        ),
        in_specs=[vmem] * (len(values) + 2),
        out_specs=(pl.BlockSpec(memory_space=pltpu.HBM), vmem),
        scratch_shapes=[
            pltpu.VMEM((1, 2, row_reach, block, breadth), jnp.float32),
            pltpu.VMEM((1, row_reach * block, breadth), jnp.float32),
            pltpu.SemaphoreType.DMA((SHIFTS, 2)),
            pltpu.SemaphoreType.DMA((SHIFTS,)),
        ],
        input_output_aliases={1: 1},
        compiler_params=pltpu.CompilerParams(vmem_limit_bytes=4 << 20),
        name="coherence",
    )(boxed, staged, *values)[0]


def solution(mesh):
    def on_device(acquired):
        return coherence(acquired.shape[2], *exchange(acquired, mesh.shape["date"], mesh.shape["tile"]))

    in_specs = (P(None, "date", ("groups", "tile"), None),)
    out_specs = P(None, None, "date", None, ("groups", "tile"), None)
    return jax.shard_map(
        on_device, mesh=mesh, in_specs=in_specs, out_specs=out_specs, check_vma=False
    )
```

```python
import functools

import jax
import jax.numpy as jnp
from jax import lax
from jax.experimental import pallas as pl
from jax.experimental.pallas import tpu as pltpu
from jax.sharding import PartitionSpec as P

SHIFTS = 4
row_reach = 5
col_reach = 2
EDGE = 8
MESH = pl.DeviceIdType.MESH


def when(*conditions):
    return pl.when(functools.reduce(jnp.logical_and, conditions))


def exchange_kernel(
    dates, tiles, mine, boxed, staged, above, rows, partial, partial_power, weights, band_out, own, core, below, relay, sums, scale,
    send, got_own, got_core, got_above, got_below, relay_send, relay_got, late_send, ready, late_ready,
):
    me = lax.axis_index("date")
    tile = lax.axis_index("tile")
    block, height, breadth = mine.shape[1:]
    near, far = dates * 5 // 16, dates * 3 // 4
    near_block, far_block = me - near, me - far
    starts = me < SHIFTS
    is_near = (near_block >= 0) & (near_block < SHIFTS)
    is_far = (far_block >= 0) & (far_block < SHIFTS - 1)

    def there(side):
        return (tile + side >= 0) & (tile + side < tiles)

    def is_first(date, at):
        return (lax.axis_index("groups") == 0) & (date == 0) & (at == 0)

    first = is_first(me, tile)
    routes = [(step, side) for step in range(SHIFTS) for side in (1, -1, 0) if (step, side) != (0, 0)]
    late = [(step, side) for step, side in routes if side < 1]

    def signal(semaphore, date, side=0):
        pl.semaphore_signal(
            semaphore, inc=1, device_id={"date": date, "tile": tile + side}, device_id_type=MESH)

    def piece(step, side, source):
        if side == 0:
            return source, core.at[step - 1], got_core.at[step - 1]
        if side == 1:
            return source.at[:, :, pl.ds(height - row_reach, row_reach), :], above.at[step, :, :, pl.ds(EDGE - row_reach, row_reach), :], got_above.at[step]
        return source.at[:, :, pl.ds(0, row_reach), :], below.at[step, :, :, pl.ds(0, row_reach), :], got_below.at[step]

    def copy(step, side, source, date, sems):
        src, dst, got = piece(step, side, source)
        return pltpu.make_async_remote_copy(
            src_ref=src, dst_ref=dst, send_sem=sems.at[step, side + 1], recv_sem=got,
            device_id={"date": date, "tile": tile + side}, device_id_type=MESH,
        )

    def straight(step, side):
        return there(side) & (me >= step) & ~is_first(me - step, tile + side)

    def around(step, side):
        return is_far & (step > far_block) & there(side)

    def to_first(step, side):
        return is_near & (near_block == step) & is_first(0, tile + side)

    barrier = pltpu.get_barrier_semaphore()
    from_first = is_first(near_block, tile)

    @pl.when(~first)
    def _():
        for step, side in routes:
            @when(there(side), me + step < dates)
            def _():
                signal(barrier, me + step, side)

            @pl.when(around(step, side))
            def _():
                signal(barrier, dates + far_block - step, side)

        for step, side in late:
            @pl.when(to_first(step, side))
            def _():
                signal(barrier, 0, side)

        @pl.when(from_first)
        def _():
            signal(barrier, 0)

        @pl.when(starts)
        def _():
            signal(barrier, me + near)

        @when(is_near, near_block < SHIFTS - 1)
        def _():
            signal(barrier, near_block + far)

        count = (is_near & ~from_first).astype(jnp.int32) + is_far.astype(jnp.int32)
        for step, side in routes:
            count += straight(step, side).astype(jnp.int32)
            count += (there(side) & (me + step >= dates)).astype(jnp.int32)
        pl.semaphore_wait(barrier, count)

    @pl.when(first)
    def _():
        pl.semaphore_wait(barrier, SHIFTS + (SHIFTS + 1 if tiles > 1 else 0))

    for step, side in routes:
        @pl.when(straight(step, side))
        def _():
            copy(step, side, mine, me - step, send).start()

    keep = pltpu.make_async_copy(mine, own, got_own)
    keep.start()

    @when(is_near, ~from_first)
    def _():
        signal(ready, near_block)

    @pl.when(is_far)
    def _():
        signal(ready, far_block + near)

    for step, side in routes:
        @when(there(side), me + step >= dates)
        def _():
            signal(ready, me + step - dates + far, side)

    for step, side in late:
        @when(first, there(-side))
        def _():
            signal(late_ready, step + near, -side)

    @pl.when(tile == 0)
    def _():
        above[...] = jnp.zeros_like(above)

    @pl.when(tile == tiles - 1)
    def _():
        below[...] = jnp.zeros_like(below)

    def to_relay(source, date):
        return pltpu.make_async_remote_copy(
            src_ref=source, dst_ref=relay, send_sem=relay_send.at[0, 1], recv_sem=relay_got,
            device_id={"date": date, "tile": tile}, device_id_type=MESH,
        )

    @pl.when(first)
    def _():
        to_relay(mine, near).start()

    @pl.when(is_far)
    def _():
        to_relay(mine, me).wait_recv()
        count = jnp.int32(0)
        for step, side in routes:
            count += around(step, side).astype(jnp.int32)
        pl.semaphore_wait(ready, count)
        for step, side in routes:
            if step:
                @pl.when(around(step, side))
                def _():
                    copy(step, side, relay, dates + far_block - step, relay_send).start()

    for step, side in reversed(routes):
        if (step, side) != (0, 1):
            @pl.when(there(-side))
            def _():
                copy(step, side, mine, me, send).wait_recv()

    keep.wait()

    band = band_table(breadth)
    band_out[...] = band
    total = height + 2 * row_reach
    above_rows = above.reshape(SHIFTS, 2, block * EDGE, breadth)
    below_rows = below.reshape(SHIFTS, 2, block * EDGE, breadth)
    own_rows = own.reshape(2, block * height, breadth)
    core_rows = core.reshape(SHIFTS - 1, 2, block * height, breadth)

    for step in range(SHIFTS):
        for part in range(2):
            for row in range(row_reach):
                rows[step, part, row_reach + height + row] = below_rows[step, part, pl.ds(row, block, stride=EDGE), :]
                if step:
                    at = pl.ds(EDGE - row_reach + row, block, stride=EDGE)
                    rows[step, part, row] = above_rows[step, part, at, :]

    for row in range(height):
        for part in range(2):
            at = pl.ds(row, block, stride=height)
            rows[0, part, row_reach + row] = own_rows[part, at, :]
            for step in range(1, SHIFTS):
                rows[step, part, row_reach + row] = core_rows[step - 1, part, at, :]

    def store(values, ref):
        for row, value in enumerate(values):
            ref[row * block:(row + 1) * block, :] = value

    for step in range(SHIFTS):
        squares = {row: square(rows, step, row) for row in range(row_reach if step == 0 else 0, total)}
        upper = inner_sums(squares, EDGE) if step == 0 else window_sums(squares, 0, EDGE)
        upper = jnp.concatenate(upper, axis=0)
        if step == 0:
            partial_power[...] = upper
        weights[step] = lax.rsqrt(box_columns(upper, band))
        store(window_sums(squares, EDGE, height), sums.at[0])
        scale[step] = lax.rsqrt(box_columns(by_date(sums.at[0], block), band)).reshape(block, EDGE, breadth)

    inner = slice(row_reach * block, EDGE * block)
    staged_rows = staged.reshape(SHIFTS, 2, block, block * EDGE, breadth)

    @pl.loop(0, SHIFTS)
    def _(step):
        upper = []
        for date in range(block):
            real, imag = products(rows, rows, step, date, range(row_reach, total))
            for part, values in enumerate((real, imag)):
                found = inner_sums(values, EDGE)
                store(found[:row_reach], partial.at[step, date, part])
                upper += found[row_reach:]
                store(window_sums(values, EDGE, height), sums.at[date * 2 + part])
        columns = box_columns(jnp.concatenate(upper, axis=0), band)
        for date in range(block):
            for row in range(row_reach, EDGE):
                weight = date_weight(weights, weights.at[step], row, date, block)
                for part in range(2):
                    at = ((date * 2 + part) * (EDGE - row_reach) + row - row_reach) * block
                    staged_rows[step, part, date, pl.ds(row, block, stride=EDGE), :] = columns[at:at + block] * weight
        for date in range(block):
            weight = scale[0, date][None] * scale[step]
            for part in range(2):
                columns = box_columns(by_date(sums.at[date * 2 + part], block), band)
                boxed[step, part, date] = columns.reshape(block, EDGE, breadth) * weight

    @when(starts, ~first)
    def _():
        pl.semaphore_wait(ready, 1)
        to_relay(mine, me + near).start()

    for step, side in late:
        @pl.when(to_first(step, side))
        def _():
            to_relay(mine, me).wait_recv()
            pl.semaphore_wait(late_ready, 1)
            copy(step, side, relay, 0, late_send).start()

    serves_first = functools.reduce(jnp.logical_or, [to_first(step, side) for step, side in late])

    @when(is_near, ~serves_first)
    def _():
        to_relay(mine, me).wait_recv()

    @when(is_near, near_block < SHIFTS - 1)
    def _():
        pl.semaphore_wait(ready, 1)
        to_relay(relay, near_block + far).start()

    for step, side in routes:
        @pl.when(straight(step, side))
        def _():
            copy(step, side, mine, me - step, send).wait_send()

        if step:
            @pl.when(around(step, side))
            def _():
                copy(step, side, relay, dates + far_block - step, relay_send).wait_send()

    for step, side in late:
        @pl.when(to_first(step, side))
        def _():
            copy(step, side, relay, 0, late_send).wait_send()

    @pl.when(starts | (is_near & (near_block < SHIFTS - 1)))
    def _():
        to_relay(mine, me).wait_send()

    @pl.when(there(-1))
    def _():
        copy(0, 1, mine, me, send).wait_recv()


def exchange(acquired, dates, tiles):
    parts, block, height, breadth = acquired.shape
    total = height + 2 * row_reach
    edge = (SHIFTS, parts, block, EDGE, breadth)
    tile = (SHIFTS, 2, block, block, EDGE, breadth)
    results = (
        tile,
        tile,
        edge,
        (SHIFTS, parts, total, block, breadth),
        (SHIFTS, block, 2, row_reach * block, breadth),
        (EDGE * block, breadth),
        (SHIFTS, EDGE * block, breadth),
    )
    return pl.pallas_call(
        functools.partial(exchange_kernel, dates, tiles),
        out_shape=tuple(jax.ShapeDtypeStruct(shape, jnp.float32) for shape in results) + (
            jax.ShapeDtypeStruct((2 * breadth, breadth), jnp.bfloat16),),
        in_specs=[pl.BlockSpec(memory_space=pltpu.HBM)],
        out_specs=(pl.BlockSpec(memory_space=pltpu.VMEM),) * (len(results) + 1),
        scratch_shapes=[
            pltpu.VMEM(acquired.shape, jnp.float32),
            pltpu.VMEM((SHIFTS - 1,) + acquired.shape, jnp.float32),
            pltpu.VMEM(edge, jnp.float32),
            pltpu.VMEM(acquired.shape, jnp.float32),
            pltpu.VMEM((2 * block, EDGE * block, breadth), jnp.float32),
            pltpu.VMEM((SHIFTS, block, EDGE, breadth), jnp.float32),
            pltpu.SemaphoreType.DMA((SHIFTS, 3)),
            pltpu.SemaphoreType.DMA,
            pltpu.SemaphoreType.DMA((SHIFTS - 1,)),
            pltpu.SemaphoreType.DMA((SHIFTS,)),
            pltpu.SemaphoreType.DMA((SHIFTS,)),
            pltpu.SemaphoreType.DMA((SHIFTS, 3)),
            pltpu.SemaphoreType.DMA,
            pltpu.SemaphoreType.DMA((SHIFTS, 3)),
            pltpu.SemaphoreType.REGULAR,
            pltpu.SemaphoreType.REGULAR,
        ],
        compiler_params=pltpu.CompilerParams(
            collective_id=0, has_side_effects=True, vmem_limit_bytes=16 << 20),
        name="exchange",
    )(pltpu.with_memory_space_constraint(acquired, pltpu.HBM))


def band_table(breadth):
    left = lax.broadcasted_iota(jnp.int32, (breadth, breadth), 0)
    right = lax.broadcasted_iota(jnp.int32, (breadth, breadth), 1)
    band = (jnp.abs(left - right) <= col_reach).astype(jnp.float32).astype(jnp.bfloat16)
    return jnp.concatenate([band, band], axis=0)


def box_columns(values, band):
    high = values.astype(jnp.bfloat16)
    low = (values - high.astype(jnp.float32)).astype(jnp.bfloat16)
    return jnp.dot(jnp.concatenate([high, low], axis=1), band, preferred_element_type=jnp.float32)


def by_date(ref, block):
    return jnp.concatenate([ref[pl.ds(date, EDGE, stride=block), :] for date in range(block)], axis=0)


def square(rows, step, row):
    real, imag = rows[step, 0, row], rows[step, 1, row]
    return real * real + imag * imag


def products(first, second, step, date, which):
    real, imag = {}, {}
    for row in which:
        second_re, second_im = second[step, 0, row], second[step, 1, row]
        first_re = jnp.broadcast_to(first[0, 0, row, pl.ds(date, 1), :], second_re.shape)
        first_im = jnp.broadcast_to(first[0, 1, row, pl.ds(date, 1), :], second_re.shape)
        real[row] = first_re * second_re + first_im * second_im
        imag[row] = first_im * second_re - first_re * second_im
    return real, imag


def window_sums(rows, start, stop):
    last = start + 2 * row_reach
    tails = {last: rows[last]}
    for row in range(last - 1, start - 1, -1):
        tails[row] = tails[row + 1] + rows[row]
    sums, head = [tails[start]], None
    for row in range(start + 1, stop):
        new = rows[row + 2 * row_reach]
        head = new if head is None else head + new
        sums.append(tails[row] + head)
    return sums


def inner_sums(rows, count):
    last = 2 * row_reach
    tails = {last: rows[last]}
    for row in range(last - 1, row_reach - 1, -1):
        tails[row] = tails[row + 1] + rows[row]
    sums, head = [tails[row_reach]], None
    for row in range(1, count):
        new = rows[row + last]
        head = new if head is None else head + new
        sums.append(tails[max(row, row_reach)] + head)
    return sums


def date_weight(first, second, row, date, block):
    return jnp.broadcast_to(first[0, pl.ds(row * block + date, 1), :], (block, second.shape[-1])) * second[pl.ds(row * block, block), :]


def coherence_kernel(
    boxed, staged_before, above, rows, partial, partial_power, weights, band, out, staged, top, found, done, done_boxed,
):
    block, height, breadth = out.shape[3:]

    def copy_boxed(step):
        return pltpu.make_async_copy(
            boxed.at[step], out.at[:, step, :, :, pl.ds(EDGE, height - EDGE), :], done_boxed.at[step])

    for step in range(SHIFTS):
        copy_boxed(step).start()
    which = range(row_reach)
    above = above.reshape(SHIFTS, 2, block * EDGE, breadth)
    staged_rows = staged.reshape(SHIFTS, 2, block, block * EDGE, breadth)

    for part in range(2):
        for row in which:
            top[0, part, row] = above[0, part, pl.ds(EDGE - row_reach + row, block, stride=EDGE), :]

    def with_top(values, inner):
        tails = [values[row_reach - 1]]
        for row in reversed(which[:-1]):
            tails.insert(0, tails[0] + values[row])
        return [tails[row] + inner[row * block:(row + 1) * block, :] for row in which]

    power = with_top({row: square(top, 0, row) for row in which}, partial_power)
    power = box_columns(jnp.concatenate(power, axis=0), band[...])
    size = block // 2

    def copy_out(step, half):
        dates = pl.ds(half * size, size)
        return pltpu.make_async_copy(
            staged.at[step, :, dates], out.at[:, step, dates, :, pl.ds(0, EDGE), :], done.at[step, half])

    def begin(step, half):
        upper = []
        for date in range(half * size, (half + 1) * size):
            both = products(top, rows if step else top, step, date, which)
            for part, values in enumerate(both):
                upper += with_top(values, partial.at[step, date, part])
        return box_columns(jnp.concatenate(upper, axis=0), band[...])

    def end(step, half, columns):
        for date in range(size):
            for row in which:
                weight = date_weight(found, weights.at[step] if step else found.at[0], row, half * size + date, block)
                for part in range(2):
                    at = ((date * 2 + part) * row_reach + row) * block
                    rows_of = pl.ds(row, block, stride=EDGE)
                    staged_rows[step, part, half * size + date, rows_of, :] = columns[at:at + block] * weight
        copy_out(step, half).start()

    pieces = [(step, half) for step in range(SHIFTS) for half in range(2)]
    begun = None
    for piece in pieces:
        columns = begin(*piece)
        if begun is None:
            found[0] = lax.rsqrt(power)
        else:
            end(*begun)
        begun = (*piece, columns)
    end(*begun)

    for step in range(SHIFTS):
        copy_boxed(step).wait()
    for piece in pieces:
        copy_out(*piece).wait()


def coherence(height, boxed, staged, *values):
    block, breadth = staged.shape[2], staged.shape[5]
    vmem = pl.BlockSpec(memory_space=pltpu.VMEM)
    return pl.pallas_call(
        coherence_kernel,
        out_shape=(
            pltpu.HBM((2, SHIFTS, block, block, height, breadth), jnp.float32),
            jax.ShapeDtypeStruct(staged.shape, jnp.float32),
        ),
        in_specs=[vmem] * (len(values) + 2),
        out_specs=(pl.BlockSpec(memory_space=pltpu.HBM), vmem),
        scratch_shapes=[
            pltpu.VMEM((1, 2, row_reach, block, breadth), jnp.float32),
            pltpu.VMEM((1, row_reach * block, breadth), jnp.float32),
            pltpu.SemaphoreType.DMA((SHIFTS, 2)),
            pltpu.SemaphoreType.DMA((SHIFTS,)),
        ],
        input_output_aliases={1: 1},
        compiler_params=pltpu.CompilerParams(vmem_limit_bytes=4 << 20),
        name="coherence",
    )(boxed, staged, *values)[0]


def solution(mesh):
    def on_device(acquired):
        return coherence(acquired.shape[2], *exchange(acquired, mesh.shape["date"], mesh.shape["tile"]))

    in_specs = (P(None, "date", ("groups", "tile"), None),)
    out_specs = P(None, None, "date", None, ("groups", "tile"), None)
    return jax.shard_map(
        on_device, mesh=mesh, in_specs=in_specs, out_specs=out_specs, check_vma=False
    )
```

```python
import functools

import jax
import jax.numpy as jnp
from jax import lax
from jax.experimental import pallas as pl
from jax.experimental.pallas import tpu as pltpu
from jax.sharding import PartitionSpec as P

SHIFTS = 4
row_reach = 5
col_reach = 2
EDGE = 8
MESH = pl.DeviceIdType.MESH


def when(*conditions):
    return pl.when(functools.reduce(jnp.logical_and, conditions))


def exchange_kernel(
    dates, tiles, mine, boxed, staged, above, rows, partial, partial_power, weights, band_out, own, core, below, relay, sums, scale,
    send, got_own, got_core, got_above, got_below, relay_got, ready, late_ready,
):
    me = lax.axis_index("date")
    tile = lax.axis_index("tile")
    block, height, breadth = mine.shape[1:]
    near, far = dates * 5 // 16, dates * 3 // 4
    near_block, far_block = me - near, me - far
    starts = me < SHIFTS
    is_near = (near_block >= 0) & (near_block < SHIFTS)
    is_far = (far_block >= 0) & (far_block < SHIFTS - 1)

    def there(side):
        return (tile + side >= 0) & (tile + side < tiles)

    def is_first(date, at):
        return (lax.axis_index("groups") == 0) & (date == 0) & (at == 0)

    first = is_first(me, tile)
    routes = [(step, side) for step in range(SHIFTS) for side in (1, -1, 0) if (step, side) != (0, 0)]
    late = [(step, side) for step, side in routes if side < 1]

    def signal(semaphore, date, side=0):
        pl.semaphore_signal(
            semaphore, inc=1, device_id={"date": date, "tile": tile + side}, device_id_type=MESH)

    def piece(step, side, source):
        if side == 0:
            return source, core.at[step - 1], got_core
        if side == 1:
            src, dst = pl.ds(height - row_reach, row_reach), pl.ds(EDGE - row_reach, row_reach)
            return source.at[:, :, src, :], above.at[step, :, :, dst, :], got_above.at[min(step, 1)]
        return source.at[:, :, pl.ds(0, row_reach), :], below.at[step, :, :, pl.ds(0, row_reach), :], got_below

    def arrived(ref, semaphore):
        pltpu.make_async_copy(ref, ref, semaphore).wait()

    def copy(step, side, source, date):
        src, dst, got = piece(step, side, source)
        return pltpu.make_async_remote_copy(
            src_ref=src, dst_ref=dst, send_sem=send.at[step, side + 1], recv_sem=got,
            device_id={"date": date, "tile": tile + side}, device_id_type=MESH,
        )

    def straight(step, side):
        return there(side) & (me >= step) & ~is_first(me - step, tile + side)

    def around(step, side):
        return is_far & (step > far_block) & there(side)

    def to_first(step, side):
        return is_near & (near_block == step) & is_first(0, tile + side)

    barrier = pltpu.get_barrier_semaphore()
    from_first = is_first(near_block, tile)

    @pl.when(~first)
    def _():
        for step, side in routes:
            @when(there(side), me + step < dates)
            def _():
                signal(barrier, me + step, side)

            @pl.when(around(step, side))
            def _():
                signal(barrier, dates + far_block - step, side)

        for step, side in late:
            @pl.when(to_first(step, side))
            def _():
                signal(barrier, 0, side)

        @pl.when(from_first)
        def _():
            signal(barrier, 0)

        @pl.when(starts)
        def _():
            signal(barrier, me + near)

        @when(is_near, near_block < SHIFTS - 1)
        def _():
            signal(barrier, near_block + far)

        count = (is_near & ~from_first).astype(jnp.int32) + is_far.astype(jnp.int32)
        for step, side in routes:
            count += straight(step, side).astype(jnp.int32)
            count += (there(side) & (me + step >= dates)).astype(jnp.int32)
        pl.semaphore_wait(barrier, count)

    @pl.when(first)
    def _():
        pl.semaphore_wait(barrier, SHIFTS + (SHIFTS + 1 if tiles > 1 else 0))

    for step, side in routes:
        @pl.when(straight(step, side))
        def _():
            copy(step, side, mine, me - step).start()

    keep = pltpu.make_async_copy(mine, own, got_own)
    keep.start()

    @when(is_near, ~from_first)
    def _():
        signal(ready, near_block)

    @pl.when(is_far)
    def _():
        signal(ready, far_block + near)

    for step, side in routes:
        @when(there(side), me + step >= dates)
        def _():
            signal(ready, me + step - dates + far, side)

    for step, side in late:
        @when(first, there(-side))
        def _():
            signal(late_ready, step + near, -side)

    @pl.when(tile == 0)
    def _():
        above[...] = jnp.zeros_like(above)

    @pl.when(tile == tiles - 1)
    def _():
        below[...] = jnp.zeros_like(below)

    def to_relay(source, date):
        return pltpu.make_async_remote_copy(
            src_ref=source, dst_ref=relay, send_sem=send.at[0, 1], recv_sem=relay_got,
            device_id={"date": date, "tile": tile}, device_id_type=MESH,
        )

    @pl.when(first)
    def _():
        to_relay(mine, near).start()

    for step, side in routes:
        @pl.when(straight(step, side))
        def _():
            copy(step, side, mine, me - step).wait_send()

    @pl.when(is_far)
    def _():
        to_relay(mine, me).wait_recv()
        count = jnp.int32(0)
        for step, side in routes:
            count += around(step, side).astype(jnp.int32)
        pl.semaphore_wait(ready, count)
        for step, side in routes:
            if step:
                @pl.when(around(step, side))
                def _():
                    copy(step, side, relay, dates + far_block - step).start()

    arrived(core, got_core)

    @pl.when(there(1))
    def _():
        arrived(below.at[:, :, :, pl.ds(0, row_reach), :], got_below)

    @pl.when(there(-1))
    def _():
        arrived(above.at[pl.ds(1, SHIFTS - 1), :, :, pl.ds(EDGE - row_reach, row_reach), :], got_above.at[1])

    keep.wait()

    band = band_table(breadth)
    band_out[...] = band
    total = height + 2 * row_reach
    above_rows = above.reshape(SHIFTS, 2, block * EDGE, breadth)
    below_rows = below.reshape(SHIFTS, 2, block * EDGE, breadth)
    own_rows = own.reshape(2, block * height, breadth)
    core_rows = core.reshape(SHIFTS - 1, 2, block * height, breadth)

    for step in range(SHIFTS):
        for part in range(2):
            for row in range(row_reach):
                rows[step, part, row_reach + height + row] = below_rows[step, part, pl.ds(row, block, stride=EDGE), :]
                if step:
                    at = pl.ds(EDGE - row_reach + row, block, stride=EDGE)
                    rows[step, part, row] = above_rows[step, part, at, :]

    for row in range(height):
        for part in range(2):
            at = pl.ds(row, block, stride=height)
            rows[0, part, row_reach + row] = own_rows[part, at, :]
            for step in range(1, SHIFTS):
                rows[step, part, row_reach + row] = core_rows[step - 1, part, at, :]

    def store(values, ref):
        for row, value in enumerate(values):
            ref[row * block:(row + 1) * block, :] = value

    for step in range(SHIFTS):
        squares = {row: square(rows, step, row) for row in range(row_reach if step == 0 else 0, total)}
        upper = inner_sums(squares, EDGE) if step == 0 else window_sums(squares, 0, EDGE)
        upper = jnp.concatenate(upper, axis=0)
        if step == 0:
            partial_power[...] = upper
        weights[step] = lax.rsqrt(box_columns(upper, band))
        store(window_sums(squares, EDGE, height), sums.at[0])
        scale[step] = lax.rsqrt(box_columns(by_date(sums.at[0], block), band)).reshape(block, EDGE, breadth)

    inner = slice(row_reach * block, EDGE * block)
    staged_rows = staged.reshape(SHIFTS, 2, block, block * EDGE, breadth)

    @pl.loop(0, SHIFTS)
    def _(step):
        upper = []
        for date in range(block):
            real, imag = products(rows, rows, step, date, range(row_reach, total))
            for part, values in enumerate((real, imag)):
                found = inner_sums(values, EDGE)
                store(found[:row_reach], partial.at[step, date, part])
                upper += found[row_reach:]
                store(window_sums(values, EDGE, height), sums.at[date * 2 + part])
        columns = box_columns(jnp.concatenate(upper, axis=0), band)
        for date in range(block):
            for row in range(row_reach, EDGE):
                weight = date_weight(weights, weights.at[step], row, date, block)
                for part in range(2):
                    at = ((date * 2 + part) * (EDGE - row_reach) + row - row_reach) * block
                    staged_rows[step, part, date, pl.ds(row, block, stride=EDGE), :] = columns[at:at + block] * weight
        for date in range(block):
            weight = scale[0, date][None] * scale[step]
            for part in range(2):
                columns = box_columns(by_date(sums.at[date * 2 + part], block), band)
                boxed[step, part, date] = columns.reshape(block, EDGE, breadth) * weight

    @when(starts, ~first)
    def _():
        pl.semaphore_wait(ready, 1)
        to_relay(mine, me + near).start()

    for step, side in late:
        @pl.when(to_first(step, side))
        def _():
            to_relay(mine, me).wait_recv()
            pl.semaphore_wait(late_ready, 1)
            copy(step, side, relay, 0).start()

    serves_first = functools.reduce(jnp.logical_or, [to_first(step, side) for step, side in late])

    @when(is_near, ~serves_first)
    def _():
        to_relay(mine, me).wait_recv()

    @when(is_near, near_block < SHIFTS - 1)
    def _():
        pl.semaphore_wait(ready, 1)
        to_relay(relay, near_block + far).start()

    for step, side in routes:
        if step:
            @pl.when(around(step, side))
            def _():
                copy(step, side, relay, dates + far_block - step).wait_send()

    for step, side in late:
        @pl.when(to_first(step, side))
        def _():
            copy(step, side, relay, 0).wait_send()

    @pl.when(starts | (is_near & (near_block < SHIFTS - 1)))
    def _():
        to_relay(mine, me).wait_send()

    @pl.when(there(-1))
    def _():
        copy(0, 1, mine, me).wait_recv()


def exchange(acquired, dates, tiles):
    parts, block, height, breadth = acquired.shape
    total = height + 2 * row_reach
    edge = (SHIFTS, parts, block, EDGE, breadth)
    tile = (SHIFTS, 2, block, block, EDGE, breadth)
    results = (
        tile,
        tile,
        edge,
        (SHIFTS, parts, total, block, breadth),
        (SHIFTS, block, 2, row_reach * block, breadth),
        (EDGE * block, breadth),
        (SHIFTS, EDGE * block, breadth),
    )
    return pl.pallas_call(
        functools.partial(exchange_kernel, dates, tiles),
        out_shape=tuple(jax.ShapeDtypeStruct(shape, jnp.float32) for shape in results) + (
            jax.ShapeDtypeStruct((2 * breadth, breadth), jnp.bfloat16),),
        in_specs=[pl.BlockSpec(memory_space=pltpu.HBM)],
        out_specs=(pl.BlockSpec(memory_space=pltpu.VMEM),) * (len(results) + 1),
        scratch_shapes=[
            pltpu.VMEM(acquired.shape, jnp.float32),
            pltpu.VMEM((SHIFTS - 1,) + acquired.shape, jnp.float32),
            pltpu.VMEM(edge, jnp.float32),
            pltpu.VMEM(acquired.shape, jnp.float32),
            pltpu.VMEM((2 * block, EDGE * block, breadth), jnp.float32),
            pltpu.VMEM((SHIFTS, block, EDGE, breadth), jnp.float32),
            pltpu.SemaphoreType.DMA((SHIFTS, 3)),
            pltpu.SemaphoreType.DMA,
            pltpu.SemaphoreType.DMA,
            pltpu.SemaphoreType.DMA((2,)),
            pltpu.SemaphoreType.DMA,
            pltpu.SemaphoreType.DMA,
            pltpu.SemaphoreType.REGULAR,
            pltpu.SemaphoreType.REGULAR,
        ],
        compiler_params=pltpu.CompilerParams(
            collective_id=0, has_side_effects=True, vmem_limit_bytes=16 << 20),
        name="exchange",
    )(pltpu.with_memory_space_constraint(acquired, pltpu.HBM))


def band_table(breadth):
    left = lax.broadcasted_iota(jnp.int32, (breadth, breadth), 0)
    right = lax.broadcasted_iota(jnp.int32, (breadth, breadth), 1)
    band = (jnp.abs(left - right) <= col_reach).astype(jnp.float32).astype(jnp.bfloat16)
    return jnp.concatenate([band, band], axis=0)


def box_columns(values, band):
    high = values.astype(jnp.bfloat16)
    low = (values - high.astype(jnp.float32)).astype(jnp.bfloat16)
    return jnp.dot(jnp.concatenate([high, low], axis=1), band, preferred_element_type=jnp.float32)


def by_date(ref, block):
    return jnp.concatenate([ref[pl.ds(date, EDGE, stride=block), :] for date in range(block)], axis=0)


def square(rows, step, row):
    real, imag = rows[step, 0, row], rows[step, 1, row]
    return real * real + imag * imag


def products(first, second, step, date, which):
    real, imag = {}, {}
    for row in which:
        second_re, second_im = second[step, 0, row], second[step, 1, row]
        first_re = jnp.broadcast_to(first[0, 0, row, pl.ds(date, 1), :], second_re.shape)
        first_im = jnp.broadcast_to(first[0, 1, row, pl.ds(date, 1), :], second_re.shape)
        real[row] = first_re * second_re + first_im * second_im
        imag[row] = first_im * second_re - first_re * second_im
    return real, imag


def window_sums(rows, start, stop):
    last = start + 2 * row_reach
    tails = {last: rows[last]}
    for row in range(last - 1, start - 1, -1):
        tails[row] = tails[row + 1] + rows[row]
    sums, head = [tails[start]], None
    for row in range(start + 1, stop):
        new = rows[row + 2 * row_reach]
        head = new if head is None else head + new
        sums.append(tails[row] + head)
    return sums


def inner_sums(rows, count):
    last = 2 * row_reach
    tails = {last: rows[last]}
    for row in range(last - 1, row_reach - 1, -1):
        tails[row] = tails[row + 1] + rows[row]
    sums, head = [tails[row_reach]], None
    for row in range(1, count):
        new = rows[row + last]
        head = new if head is None else head + new
        sums.append(tails[max(row, row_reach)] + head)
    return sums


def date_weight(first, second, row, date, block):
    return jnp.broadcast_to(first[0, pl.ds(row * block + date, 1), :], (block, second.shape[-1])) * second[pl.ds(row * block, block), :]


def coherence_kernel(
    boxed, staged_before, above, rows, partial, partial_power, weights, band, out, staged, top, found, done,
):
    block, height, breadth = out.shape[3:]

    def copy_boxed(step):
        return pltpu.make_async_copy(
            boxed.at[step], out.at[:, step, :, :, pl.ds(EDGE, height - EDGE), :], done)

    for step in range(SHIFTS):
        copy_boxed(step).start()
    which = range(row_reach)
    above = above.reshape(SHIFTS, 2, block * EDGE, breadth)
    staged_rows = staged.reshape(SHIFTS, 2, block, block * EDGE, breadth)

    for part in range(2):
        for row in which:
            top[0, part, row] = above[0, part, pl.ds(EDGE - row_reach + row, block, stride=EDGE), :]

    def with_top(values, inner):
        tails = [values[row_reach - 1]]
        for row in reversed(which[:-1]):
            tails.insert(0, tails[0] + values[row])
        return [tails[row] + inner[row * block:(row + 1) * block, :] for row in which]

    power = with_top({row: square(top, 0, row) for row in which}, partial_power)
    power = box_columns(jnp.concatenate(power, axis=0), band[...])
    size = block // 2

    def copy_out(step, half):
        dates = pl.ds(half * size, size)
        return pltpu.make_async_copy(
            staged.at[step, :, dates], out.at[:, step, dates, :, pl.ds(0, EDGE), :], done)

    def begin(step, half):
        upper = []
        for date in range(half * size, (half + 1) * size):
            both = products(top, rows if step else top, step, date, which)
            for part, values in enumerate(both):
                upper += with_top(values, partial.at[step, date, part])
        return box_columns(jnp.concatenate(upper, axis=0), band[...])

    def end(step, half, columns):
        for date in range(size):
            for row in which:
                weight = date_weight(found, weights.at[step] if step else found.at[0], row, half * size + date, block)
                for part in range(2):
                    at = ((date * 2 + part) * row_reach + row) * block
                    rows_of = pl.ds(row, block, stride=EDGE)
                    staged_rows[step, part, half * size + date, rows_of, :] = columns[at:at + block] * weight
        copy_out(step, half).start()

    pieces = [(step, half) for step in range(SHIFTS) for half in range(2)]
    begun = None
    for piece in pieces:
        columns = begin(*piece)
        if begun is None:
            found[0] = lax.rsqrt(power)
        else:
            end(*begun)
        begun = (*piece, columns)
    end(*begun)

    pltpu.make_async_copy(out, out, done).wait()


def coherence(height, boxed, staged, *values):
    block, breadth = staged.shape[2], staged.shape[5]
    vmem = pl.BlockSpec(memory_space=pltpu.VMEM)
    return pl.pallas_call(
        coherence_kernel,
        out_shape=(
            pltpu.HBM((2, SHIFTS, block, block, height, breadth), jnp.float32),
            jax.ShapeDtypeStruct(staged.shape, jnp.float32),
        ),
        in_specs=[vmem] * (len(values) + 2),
        out_specs=(pl.BlockSpec(memory_space=pltpu.HBM), vmem),
        scratch_shapes=[
            pltpu.VMEM((1, 2, row_reach, block, breadth), jnp.float32),
            pltpu.VMEM((1, row_reach * block, breadth), jnp.float32),
            pltpu.SemaphoreType.DMA,
        ],
        input_output_aliases={1: 1},
        compiler_params=pltpu.CompilerParams(vmem_limit_bytes=4 << 20),
        name="coherence",
    )(boxed, staged, *values)[0]


def solution(mesh):
    def on_device(acquired):
        return coherence(acquired.shape[2], *exchange(acquired, mesh.shape["date"], mesh.shape["tile"]))

    in_specs = (P(None, "date", ("groups", "tile"), None),)
    out_specs = P(None, None, "date", None, ("groups", "tile"), None)
    return jax.shard_map(
        on_device, mesh=mesh, in_specs=in_specs, out_specs=out_specs, check_vma=False
    )
```

```python
import functools

import jax
import jax.numpy as jnp
from jax import lax
from jax.experimental import pallas as pl
from jax.experimental.pallas import tpu as pltpu
from jax.sharding import PartitionSpec as P

SHIFTS = 4
row_reach = 5
col_reach = 2
EDGE = 8
MESH = pl.DeviceIdType.MESH


def when(*conditions):
    return pl.when(functools.reduce(jnp.logical_and, conditions))


def exchange_kernel(
    dates, tiles, mine, boxed, staged, above, rows, partial, partial_power, weights, band_out, own, core, below, relay, sums, scale,
    send, got_own, got_core, got_above, got_below, relay_got, ready, late_ready,
):
    me = lax.axis_index("date")
    tile = lax.axis_index("tile")
    block, height, breadth = mine.shape[1:]
    near, far = dates * 5 // 16, dates * 3 // 4
    near_block, far_block = me - near, me - far
    starts = me < SHIFTS
    is_near = (near_block >= 0) & (near_block < SHIFTS)
    is_far = (far_block >= 0) & (far_block < SHIFTS - 1)

    def there(side):
        return (tile + side >= 0) & (tile + side < tiles)

    def is_first(date, at):
        return (lax.axis_index("groups") == 0) & (date == 0) & (at == 0)

    first = is_first(me, tile)
    routes = [(step, side) for step in range(SHIFTS) for side in (1, -1, 0) if (step, side) != (0, 0)]
    late = [(step, side) for step, side in routes if side < 1]

    def signal(semaphore, date, side=0):
        pl.semaphore_signal(
            semaphore, inc=1, device_id={"date": date, "tile": tile + side}, device_id_type=MESH)

    def piece(step, side, source):
        if side == 0:
            return source, core.at[step - 1], got_core
        if side == 1:
            src, dst = pl.ds(height - row_reach, row_reach), pl.ds(EDGE - row_reach, row_reach)
            return source.at[:, :, src, :], above.at[step, :, :, dst, :], got_above.at[min(step, 1)]
        return source.at[:, :, pl.ds(0, row_reach), :], below.at[step, :, :, pl.ds(0, row_reach), :], got_below

    def arrived(ref, semaphore):
        pltpu.make_async_copy(ref, ref, semaphore).wait()

    def copy(step, side, source, date):
        src, dst, got = piece(step, side, source)
        return pltpu.make_async_remote_copy(
            src_ref=src, dst_ref=dst, send_sem=send.at[side % 4], recv_sem=got,
            device_id={"date": date, "tile": tile + side}, device_id_type=MESH,
        )

    def straight(step, side):
        return there(side) & (me >= step) & ~is_first(me - step, tile + side)

    def around(step, side):
        return is_far & (step > far_block) & there(side)

    def to_first(step, side):
        return is_near & (near_block == step) & is_first(0, tile + side)

    barrier = pltpu.get_barrier_semaphore()
    from_first = is_first(near_block, tile)

    @pl.when(~first)
    def _():
        for step, side in routes:
            @when(there(side), me + step < dates)
            def _():
                signal(barrier, me + step, side)

            @pl.when(around(step, side))
            def _():
                signal(barrier, dates + far_block - step, side)

        for step, side in late:
            @pl.when(to_first(step, side))
            def _():
                signal(barrier, 0, side)

        @pl.when(from_first)
        def _():
            signal(barrier, 0)

        @pl.when(starts)
        def _():
            signal(barrier, me + near)

        @when(is_near, near_block < SHIFTS - 1)
        def _():
            signal(barrier, near_block + far)

        count = (is_near & ~from_first).astype(jnp.int32) + is_far.astype(jnp.int32)
        for step, side in routes:
            count += straight(step, side).astype(jnp.int32)
            count += (there(side) & (me + step >= dates)).astype(jnp.int32)
        pl.semaphore_wait(barrier, count)

    @pl.when(first)
    def _():
        pl.semaphore_wait(barrier, SHIFTS + (SHIFTS + 1 if tiles > 1 else 0))

    for step in range(SHIFTS):
        sides = [side for at, side in routes if at == step]
        for side in sides:
            @pl.when(straight(step, side))
            def _():
                copy(step, side, mine, me - step).start()

        for side in sides:
            @when(straight(step, side), starts)
            def _():
                copy(step, side, mine, me - step).wait_send()

    keep = pltpu.make_async_copy(mine, own, got_own)
    keep.start()

    @when(is_near, ~from_first)
    def _():
        signal(ready, near_block)

    @pl.when(is_far)
    def _():
        signal(ready, far_block + near)

    for step, side in routes:
        @when(there(side), me + step >= dates)
        def _():
            signal(ready, me + step - dates + far, side)

    for step, side in late:
        @when(first, there(-side))
        def _():
            signal(late_ready, step + near, -side)

    @pl.when(tile == 0)
    def _():
        above[...] = jnp.zeros_like(above)

    @pl.when(tile == tiles - 1)
    def _():
        below[...] = jnp.zeros_like(below)

    def to_relay(source, date):
        return pltpu.make_async_remote_copy(
            src_ref=source, dst_ref=relay, send_sem=send.at[2], recv_sem=relay_got,
            device_id={"date": date, "tile": tile}, device_id_type=MESH,
        )

    @pl.when(first)
    def _():
        to_relay(mine, near).start()

    edges = above.at[:, :, :, pl.ds(EDGE - row_reach, row_reach), :]
    for side, sent in ((1, edges), (-1, edges), (0, core)):
        @when(~starts, there(side))
        def _():
            arrived(sent, send.at[side % 4])

    @pl.when(is_far)
    def _():
        to_relay(mine, me).wait_recv()
        count = jnp.int32(0)
        for step, side in routes:
            count += around(step, side).astype(jnp.int32)
        pl.semaphore_wait(ready, count)
        for step in range(1, SHIFTS):
            for side in (1, -1, 0):
                @pl.when(around(step, side))
                def _():
                    copy(step, side, relay, dates + far_block - step).start()

            for side in (1, -1, 0):
                @pl.when(around(step, side))
                def _():
                    copy(step, side, relay, dates + far_block - step).wait_send()

    arrived(core, got_core)

    @pl.when(there(1))
    def _():
        arrived(below.at[:, :, :, pl.ds(0, row_reach), :], got_below)

    @pl.when(there(-1))
    def _():
        arrived(above.at[pl.ds(1, SHIFTS - 1), :, :, pl.ds(EDGE - row_reach, row_reach), :], got_above.at[1])

    keep.wait()

    band = band_table(breadth)
    band_out[...] = band
    total = height + 2 * row_reach
    above_rows = above.reshape(SHIFTS, 2, block * EDGE, breadth)
    below_rows = below.reshape(SHIFTS, 2, block * EDGE, breadth)
    own_rows = own.reshape(2, block * height, breadth)
    core_rows = core.reshape(SHIFTS - 1, 2, block * height, breadth)

    for step in range(SHIFTS):
        for part in range(2):
            for row in range(row_reach):
                rows[step, part, row_reach + height + row] = below_rows[step, part, pl.ds(row, block, stride=EDGE), :]
                if step:
                    at = pl.ds(EDGE - row_reach + row, block, stride=EDGE)
                    rows[step, part, row] = above_rows[step, part, at, :]

    for row in range(height):
        for part in range(2):
            at = pl.ds(row, block, stride=height)
            rows[0, part, row_reach + row] = own_rows[part, at, :]
            for step in range(1, SHIFTS):
                rows[step, part, row_reach + row] = core_rows[step - 1, part, at, :]

    def store(values, ref):
        for row, value in enumerate(values):
            ref[row * block:(row + 1) * block, :] = value

    for step in range(SHIFTS):
        squares = {row: square(rows, step, row) for row in range(row_reach if step == 0 else 0, total)}
        upper = inner_sums(squares, EDGE) if step == 0 else window_sums(squares, 0, EDGE)
        upper = jnp.concatenate(upper, axis=0)
        if step == 0:
            partial_power[...] = upper
        weights[step] = lax.rsqrt(box_columns(upper, band))
        store(window_sums(squares, EDGE, height), sums.at[0])
        scale[step] = lax.rsqrt(box_columns(by_date(sums.at[0], block), band)).reshape(block, EDGE, breadth)

    inner = slice(row_reach * block, EDGE * block)
    staged_rows = staged.reshape(SHIFTS, 2, block, block * EDGE, breadth)

    @pl.loop(0, SHIFTS)
    def _(step):
        upper = []
        for date in range(block):
            real, imag = products(rows, rows, step, date, range(row_reach, total))
            for part, values in enumerate((real, imag)):
                found = inner_sums(values, EDGE)
                store(found[:row_reach], partial.at[step, date, part])
                upper += found[row_reach:]
                store(window_sums(values, EDGE, height), sums.at[date * 2 + part])
        columns = box_columns(jnp.concatenate(upper, axis=0), band)
        for date in range(block):
            for row in range(row_reach, EDGE):
                weight = date_weight(weights, weights.at[step], row, date, block)
                for part in range(2):
                    at = ((date * 2 + part) * (EDGE - row_reach) + row - row_reach) * block
                    staged_rows[step, part, date, pl.ds(row, block, stride=EDGE), :] = columns[at:at + block] * weight
        for date in range(block):
            weight = scale[0, date][None] * scale[step]
            for part in range(2):
                columns = box_columns(by_date(sums.at[date * 2 + part], block), band)
                boxed[step, part, date] = columns.reshape(block, EDGE, breadth) * weight

    @when(starts, ~first)
    def _():
        pl.semaphore_wait(ready, 1)
        to_relay(mine, me + near).start()

    for step, side in late:
        @pl.when(to_first(step, side))
        def _():
            to_relay(mine, me).wait_recv()
            pl.semaphore_wait(late_ready, 1)
            copy(step, side, relay, 0).start()

    serves_first = functools.reduce(jnp.logical_or, [to_first(step, side) for step, side in late])

    @when(is_near, ~serves_first)
    def _():
        to_relay(mine, me).wait_recv()

    @when(is_near, near_block < SHIFTS - 1)
    def _():
        pl.semaphore_wait(ready, 1)
        to_relay(relay, near_block + far).start()

    for step, side in late:
        @pl.when(to_first(step, side))
        def _():
            copy(step, side, relay, 0).wait_send()

    @pl.when(starts | (is_near & (near_block < SHIFTS - 1)))
    def _():
        to_relay(mine, me).wait_send()

    @pl.when(there(-1))
    def _():
        copy(0, 1, mine, me).wait_recv()


def exchange(acquired, dates, tiles):
    parts, block, height, breadth = acquired.shape
    total = height + 2 * row_reach
    edge = (SHIFTS, parts, block, EDGE, breadth)
    tile = (SHIFTS, 2, block, block, EDGE, breadth)
    results = (
        tile,
        tile,
        edge,
        (SHIFTS, parts, total, block, breadth),
        (SHIFTS, block, 2, row_reach * block, breadth),
        (EDGE * block, breadth),
        (SHIFTS, EDGE * block, breadth),
    )
    return pl.pallas_call(
        functools.partial(exchange_kernel, dates, tiles),
        out_shape=tuple(jax.ShapeDtypeStruct(shape, jnp.float32) for shape in results) + (
            jax.ShapeDtypeStruct((2 * breadth, breadth), jnp.bfloat16),),
        in_specs=[pl.BlockSpec(memory_space=pltpu.HBM)],
        out_specs=(pl.BlockSpec(memory_space=pltpu.VMEM),) * (len(results) + 1),
        scratch_shapes=[
            pltpu.VMEM(acquired.shape, jnp.float32),
            pltpu.VMEM((SHIFTS - 1,) + acquired.shape, jnp.float32),
            pltpu.VMEM(edge, jnp.float32),
            pltpu.VMEM(acquired.shape, jnp.float32),
            pltpu.VMEM((2 * block, EDGE * block, breadth), jnp.float32),
            pltpu.VMEM((SHIFTS, block, EDGE, breadth), jnp.float32),
            pltpu.SemaphoreType.DMA((4,)),
            pltpu.SemaphoreType.DMA,
            pltpu.SemaphoreType.DMA,
            pltpu.SemaphoreType.DMA((2,)),
            pltpu.SemaphoreType.DMA,
            pltpu.SemaphoreType.DMA,
            pltpu.SemaphoreType.REGULAR,
            pltpu.SemaphoreType.REGULAR,
        ],
        compiler_params=pltpu.CompilerParams(
            collective_id=0, has_side_effects=True, vmem_limit_bytes=16 << 20),
        name="exchange",
    )(pltpu.with_memory_space_constraint(acquired, pltpu.HBM))


def band_table(breadth):
    left = lax.broadcasted_iota(jnp.int32, (breadth, breadth), 0)
    right = lax.broadcasted_iota(jnp.int32, (breadth, breadth), 1)
    band = (jnp.abs(left - right) <= col_reach).astype(jnp.float32).astype(jnp.bfloat16)
    return jnp.concatenate([band, band], axis=0)


def box_columns(values, band):
    high = values.astype(jnp.bfloat16)
    low = (values - high.astype(jnp.float32)).astype(jnp.bfloat16)
    return jnp.dot(jnp.concatenate([high, low], axis=1), band, preferred_element_type=jnp.float32)


def by_date(ref, block):
    return jnp.concatenate([ref[pl.ds(date, EDGE, stride=block), :] for date in range(block)], axis=0)


def square(rows, step, row):
    real, imag = rows[step, 0, row], rows[step, 1, row]
    return real * real + imag * imag


def products(first, second, step, date, which):
    real, imag = {}, {}
    for row in which:
        second_re, second_im = second[step, 0, row], second[step, 1, row]
        first_re = jnp.broadcast_to(first[0, 0, row, pl.ds(date, 1), :], second_re.shape)
        first_im = jnp.broadcast_to(first[0, 1, row, pl.ds(date, 1), :], second_re.shape)
        real[row] = first_re * second_re + first_im * second_im
        imag[row] = first_im * second_re - first_re * second_im
    return real, imag


def window_sums(rows, start, stop):
    last = start + 2 * row_reach
    tails = {last: rows[last]}
    for row in range(last - 1, start - 1, -1):
        tails[row] = tails[row + 1] + rows[row]
    sums, head = [tails[start]], None
    for row in range(start + 1, stop):
        new = rows[row + 2 * row_reach]
        head = new if head is None else head + new
        sums.append(tails[row] + head)
    return sums


def inner_sums(rows, count):
    last = 2 * row_reach
    tails = {last: rows[last]}
    for row in range(last - 1, row_reach - 1, -1):
        tails[row] = tails[row + 1] + rows[row]
    sums, head = [tails[row_reach]], None
    for row in range(1, count):
        new = rows[row + last]
        head = new if head is None else head + new
        sums.append(tails[max(row, row_reach)] + head)
    return sums


def date_weight(first, second, row, date, block):
    return jnp.broadcast_to(first[0, pl.ds(row * block + date, 1), :], (block, second.shape[-1])) * second[pl.ds(row * block, block), :]


def coherence_kernel(
    boxed, staged_before, above, rows, partial, partial_power, weights, band, out, staged, top, found, done,
):
    block, height, breadth = out.shape[3:]

    def copy_boxed(step):
        return pltpu.make_async_copy(
            boxed.at[step], out.at[:, step, :, :, pl.ds(EDGE, height - EDGE), :], done)

    for step in range(SHIFTS):
        copy_boxed(step).start()
    which = range(row_reach)
    above = above.reshape(SHIFTS, 2, block * EDGE, breadth)
    staged_rows = staged.reshape(SHIFTS, 2, block, block * EDGE, breadth)

    for part in range(2):
        for row in which:
            top[0, part, row] = above[0, part, pl.ds(EDGE - row_reach + row, block, stride=EDGE), :]

    def with_top(values, inner):
        tails = [values[row_reach - 1]]
        for row in reversed(which[:-1]):
            tails.insert(0, tails[0] + values[row])
        return [tails[row] + inner[row * block:(row + 1) * block, :] for row in which]

    power = with_top({row: square(top, 0, row) for row in which}, partial_power)
    power = box_columns(jnp.concatenate(power, axis=0), band[...])
    size = block // 2

    def copy_out(step, half):
        dates = pl.ds(half * size, size)
        return pltpu.make_async_copy(
            staged.at[step, :, dates], out.at[:, step, dates, :, pl.ds(0, EDGE), :], done)

    def begin(step, half):
        upper = []
        for date in range(half * size, (half + 1) * size):
            both = products(top, rows if step else top, step, date, which)
            for part, values in enumerate(both):
                upper += with_top(values, partial.at[step, date, part])
        return box_columns(jnp.concatenate(upper, axis=0), band[...])

    def end(step, half, columns):
        for date in range(size):
            for row in which:
                weight = date_weight(found, weights.at[step] if step else found.at[0], row, half * size + date, block)
                for part in range(2):
                    at = ((date * 2 + part) * row_reach + row) * block
                    rows_of = pl.ds(row, block, stride=EDGE)
                    staged_rows[step, part, half * size + date, rows_of, :] = columns[at:at + block] * weight
        copy_out(step, half).start()

    pieces = [(step, half) for step in range(SHIFTS) for half in range(2)]
    begun = None
    for piece in pieces:
        columns = begin(*piece)
        if begun is None:
            found[0] = lax.rsqrt(power)
        else:
            end(*begun)
        begun = (*piece, columns)
    end(*begun)

    pltpu.make_async_copy(out, out, done).wait()


def coherence(height, boxed, staged, *values):
    block, breadth = staged.shape[2], staged.shape[5]
    vmem = pl.BlockSpec(memory_space=pltpu.VMEM)
    return pl.pallas_call(
        coherence_kernel,
        out_shape=(
            pltpu.HBM((2, SHIFTS, block, block, height, breadth), jnp.float32),
            jax.ShapeDtypeStruct(staged.shape, jnp.float32),
        ),
        in_specs=[vmem] * (len(values) + 2),
        out_specs=(pl.BlockSpec(memory_space=pltpu.HBM), vmem),
        scratch_shapes=[
            pltpu.VMEM((1, 2, row_reach, block, breadth), jnp.float32),
            pltpu.VMEM((1, row_reach * block, breadth), jnp.float32),
            pltpu.SemaphoreType.DMA,
        ],
        input_output_aliases={1: 1},
        compiler_params=pltpu.CompilerParams(vmem_limit_bytes=4 << 20),
        name="coherence",
    )(boxed, staged, *values)[0]


def solution(mesh):
    def on_device(acquired):
        return coherence(acquired.shape[2], *exchange(acquired, mesh.shape["date"], mesh.shape["tile"]))

    in_specs = (P(None, "date", ("groups", "tile"), None),)
    out_specs = P(None, None, "date", None, ("groups", "tile"), None)
    return jax.shard_map(
        on_device, mesh=mesh, in_specs=in_specs, out_specs=out_specs, check_vma=False
    )
```

```python
import functools

import jax
import jax.numpy as jnp
from jax import lax
from jax.experimental import pallas as pl
from jax.experimental.pallas import tpu as pltpu
from jax.sharding import PartitionSpec as P

SHIFTS = 4
row_reach = 5
col_reach = 2
EDGE = 8
MESH = pl.DeviceIdType.MESH


def when(*conditions):
    return pl.when(functools.reduce(jnp.logical_and, conditions))


def exchange_kernel(
    dates, tiles, mine, boxed, staged, above, rows, partial, partial_power, weights, band_out, core, below, relay, sums, scale,
    send, got_core, got_above, got_below, relay_got, ready,
):
    me = lax.axis_index("date")
    tile = lax.axis_index("tile")
    block, height, breadth = mine.shape[1:]
    near, far = dates * 5 // 16, dates * 3 // 4
    near_block, far_block = me - near, me - far
    starts = me < SHIFTS
    is_near = (near_block >= 0) & (near_block < SHIFTS)
    is_far = (far_block >= 0) & (far_block < SHIFTS - 1)

    def there(side):
        return (tile + side >= 0) & (tile + side < tiles)

    def is_first(date, at):
        return (lax.axis_index("groups") == 0) & (date == 0) & (at == 0)

    first = is_first(me, tile)
    routes = [(step, side) for step in range(SHIFTS) for side in (1, -1, 0) if (step, side) != (0, 0)]
    late = [(step, side) for step, side in routes if side < 1]

    def signal(semaphore, date, side=0):
        pl.semaphore_signal(
            semaphore, inc=1, device_id={"date": date, "tile": tile + side}, device_id_type=MESH)

    def piece(step, side, source):
        if side == 0:
            return source, core.at[step], got_core
        if side == 1:
            src, dst = pl.ds(height - row_reach, row_reach), pl.ds(EDGE - row_reach, row_reach)
            return source.at[:, :, src, :], above.at[step, :, :, dst, :], got_above.at[min(step, 1)]
        return source.at[:, :, pl.ds(0, row_reach), :], below.at[step, :, :, pl.ds(0, row_reach), :], got_below

    def arrived(ref, semaphore):
        pltpu.make_async_copy(ref, ref, semaphore).wait()

    def copy(step, side, source, date):
        src, dst, got = piece(step, side, source)
        return pltpu.make_async_remote_copy(
            src_ref=src, dst_ref=dst, send_sem=send.at[side % 3], recv_sem=got,
            device_id={"date": date, "tile": tile + side}, device_id_type=MESH,
        )

    def straight(step, side):
        return there(side) & (me >= step) & ~is_first(me - step, tile + side)

    def around(step, side):
        return is_far & (step > far_block) & there(side)

    def to_first(step, side):
        return is_near & (near_block == step) & is_first(0, tile + side)

    barrier = pltpu.get_barrier_semaphore()
    from_first = is_first(near_block, tile)

    @pl.when(~first)
    def _():
        for step, side in routes:
            @when(there(side), me + step < dates)
            def _():
                signal(barrier, me + step, side)

            @pl.when(around(step, side))
            def _():
                signal(barrier, dates + far_block - step, side)

        for step, side in late:
            @pl.when(to_first(step, side))
            def _():
                signal(barrier, 0, side)

        @pl.when(from_first)
        def _():
            signal(barrier, 0)

        @pl.when(starts)
        def _():
            signal(barrier, me + near)

        @when(is_near, near_block < SHIFTS - 1)
        def _():
            signal(barrier, near_block + far)

        count = (is_near & ~from_first).astype(jnp.int32) + is_far.astype(jnp.int32)
        for step, side in routes:
            count += straight(step, side).astype(jnp.int32)
            count += (there(side) & (me + step >= dates)).astype(jnp.int32)
        pl.semaphore_wait(barrier, count)

    @pl.when(first)
    def _():
        pl.semaphore_wait(barrier, SHIFTS + (SHIFTS + 1 if tiles > 1 else 0))

    for step in range(SHIFTS):
        sides = [side for at, side in routes if at == step]
        for side in sides:
            @pl.when(straight(step, side))
            def _():
                copy(step, side, mine, me - step).start()

        for side in sides:
            @when(straight(step, side), starts)
            def _():
                copy(step, side, mine, me - step).wait_send()

    pltpu.make_async_copy(mine, core.at[0], got_core).start()

    @when(is_near, ~from_first)
    def _():
        signal(ready, near_block)

    @pl.when(is_far)
    def _():
        signal(ready, far_block + near)

    for step, side in routes:
        @when(there(side), me + step >= dates)
        def _():
            signal(ready, me + step - dates + far, side)

    for step, side in late:
        @when(first, there(-side))
        def _():
            signal(ready, step + near, -side)

    @pl.when(tile == 0)
    def _():
        above[...] = jnp.zeros_like(above)

    @pl.when(tile == tiles - 1)
    def _():
        below[...] = jnp.zeros_like(below)

    def to_relay(source, date):
        return pltpu.make_async_remote_copy(
            src_ref=source, dst_ref=relay, send_sem=send.at[1], recv_sem=relay_got,
            device_id={"date": date, "tile": tile}, device_id_type=MESH,
        )

    @pl.when(first)
    def _():
        to_relay(mine, near).start()

    edges = above.at[:, :, :, pl.ds(EDGE - row_reach, row_reach), :]
    for side, sent in ((1, edges), (-1, edges), (0, core.at[pl.ds(1, SHIFTS - 1)])):
        @when(~starts, there(side))
        def _():
            arrived(sent, send.at[side % 3])

    @pl.when(is_far)
    def _():
        to_relay(mine, me).wait_recv()
        count = jnp.int32(0)
        for step, side in routes:
            count += around(step, side).astype(jnp.int32)
        pl.semaphore_wait(ready, count)
        for step in range(1, SHIFTS):
            for side in (1, -1, 0):
                @pl.when(around(step, side))
                def _():
                    copy(step, side, relay, dates + far_block - step).start()

            for side in (1, -1, 0):
                @pl.when(around(step, side))
                def _():
                    copy(step, side, relay, dates + far_block - step).wait_send()

    arrived(core, got_core)

    @pl.when(there(1))
    def _():
        arrived(below.at[:, :, :, pl.ds(0, row_reach), :], got_below)

    @pl.when(there(-1))
    def _():
        arrived(above.at[pl.ds(1, SHIFTS - 1), :, :, pl.ds(EDGE - row_reach, row_reach), :], got_above.at[1])

    band = band_table(breadth)
    band_out[...] = band
    total = height + 2 * row_reach
    above_rows = above.reshape(SHIFTS, 2, block * EDGE, breadth)
    below_rows = below.reshape(SHIFTS, 2, block * EDGE, breadth)
    core_rows = core.reshape(SHIFTS, 2, block * height, breadth)

    for step in range(SHIFTS):
        for part in range(2):
            for row in range(row_reach):
                rows[step, part, row_reach + height + row] = below_rows[step, part, pl.ds(row, block, stride=EDGE), :]
                if step:
                    at = pl.ds(EDGE - row_reach + row, block, stride=EDGE)
                    rows[step, part, row] = above_rows[step, part, at, :]

    for row in range(height):
        for part in range(2):
            at = pl.ds(row, block, stride=height)
            for step in range(SHIFTS):
                rows[step, part, row_reach + row] = core_rows[step, part, at, :]

    def store(values, ref):
        for row, value in enumerate(values):
            ref[row * block:(row + 1) * block, :] = value

    for step in range(SHIFTS):
        squares = {row: square(rows, step, row) for row in range(row_reach if step == 0 else 0, total)}
        upper = inner_sums(squares, EDGE) if step == 0 else window_sums(squares, 0, EDGE)
        upper = jnp.concatenate(upper, axis=0)
        if step == 0:
            partial_power[...] = upper
        weights[step] = lax.rsqrt(box_columns(upper, band))
        store(window_sums(squares, EDGE, height), sums.at[0])
        scale[step] = lax.rsqrt(box_columns(by_date(sums.at[0], block), band)).reshape(block, EDGE, breadth)

    inner = slice(row_reach * block, EDGE * block)
    staged_rows = staged.reshape(SHIFTS, 2, block, block * EDGE, breadth)

    @pl.loop(0, SHIFTS)
    def _(step):
        upper = []
        for date in range(block):
            real, imag = products(rows, rows, step, date, range(row_reach, total))
            for part, values in enumerate((real, imag)):
                found = inner_sums(values, EDGE)
                store(found[:row_reach], partial.at[step, date, part])
                upper += found[row_reach:]
                store(window_sums(values, EDGE, height), sums.at[date * 2 + part])
        columns = box_columns(jnp.concatenate(upper, axis=0), band)
        for date in range(block):
            for row in range(row_reach, EDGE):
                weight = date_weight(weights, weights.at[step], row, date, block)
                for part in range(2):
                    at = ((date * 2 + part) * (EDGE - row_reach) + row - row_reach) * block
                    staged_rows[step, part, date, pl.ds(row, block, stride=EDGE), :] = columns[at:at + block] * weight
        for date in range(block):
            weight = scale[0, date][None] * scale[step]
            for part in range(2):
                columns = box_columns(by_date(sums.at[date * 2 + part], block), band)
                boxed[step, part, date] = columns.reshape(block, EDGE, breadth) * weight

    @when(starts, ~first)
    def _():
        pl.semaphore_wait(ready, 1)
        to_relay(mine, me + near).start()

    passes_on = is_near & (near_block < SHIFTS - 1)

    @pl.when(is_near)
    def _():
        to_relay(mine, me).wait_recv()
        count = passes_on.astype(jnp.int32)
        for step, side in late:
            count += to_first(step, side).astype(jnp.int32)

        @pl.when(count > 0)
        def _():
            pl.semaphore_wait(ready, count)

    for step, side in late:
        @pl.when(to_first(step, side))
        def _():
            copy(step, side, relay, 0).start()

    @pl.when(passes_on)
    def _():
        to_relay(relay, near_block + far).start()

    for step, side in late:
        @pl.when(to_first(step, side))
        def _():
            copy(step, side, relay, 0).wait_send()

    @pl.when(starts | (is_near & (near_block < SHIFTS - 1)))
    def _():
        to_relay(mine, me).wait_send()

    @pl.when(there(-1))
    def _():
        copy(0, 1, mine, me).wait_recv()


def exchange(acquired, dates, tiles):
    parts, block, height, breadth = acquired.shape
    total = height + 2 * row_reach
    edge = (SHIFTS, parts, block, EDGE, breadth)
    tile = (SHIFTS, 2, block, block, EDGE, breadth)
    results = (
        tile,
        tile,
        edge,
        (SHIFTS, parts, total, block, breadth),
        (SHIFTS, block, 2, row_reach * block, breadth),
        (EDGE * block, breadth),
        (SHIFTS, EDGE * block, breadth),
    )
    return pl.pallas_call(
        functools.partial(exchange_kernel, dates, tiles),
        out_shape=tuple(jax.ShapeDtypeStruct(shape, jnp.float32) for shape in results) + (
            jax.ShapeDtypeStruct((2 * breadth, breadth), jnp.bfloat16),),
        in_specs=[pl.BlockSpec(memory_space=pltpu.HBM)],
        out_specs=(pl.BlockSpec(memory_space=pltpu.VMEM),) * (len(results) + 1),
        scratch_shapes=[
            pltpu.VMEM((SHIFTS,) + acquired.shape, jnp.float32),
            pltpu.VMEM(edge, jnp.float32),
            pltpu.VMEM(acquired.shape, jnp.float32),
            pltpu.VMEM((2 * block, EDGE * block, breadth), jnp.float32),
            pltpu.VMEM((SHIFTS, block, EDGE, breadth), jnp.float32),
            pltpu.SemaphoreType.DMA((3,)),
            pltpu.SemaphoreType.DMA,
            pltpu.SemaphoreType.DMA((2,)),
            pltpu.SemaphoreType.DMA,
            pltpu.SemaphoreType.DMA,
            pltpu.SemaphoreType.REGULAR,
        ],
        compiler_params=pltpu.CompilerParams(
            collective_id=0, has_side_effects=True, vmem_limit_bytes=16 << 20),
        name="exchange",
    )(pltpu.with_memory_space_constraint(acquired, pltpu.HBM))


def band_table(breadth):
    left = lax.broadcasted_iota(jnp.int32, (breadth, breadth), 0)
    right = lax.broadcasted_iota(jnp.int32, (breadth, breadth), 1)
    band = (jnp.abs(left - right) <= col_reach).astype(jnp.float32).astype(jnp.bfloat16)
    return jnp.concatenate([band, band], axis=0)


def box_columns(values, band):
    high = values.astype(jnp.bfloat16)
    low = (values - high.astype(jnp.float32)).astype(jnp.bfloat16)
    return jnp.dot(jnp.concatenate([high, low], axis=1), band, preferred_element_type=jnp.float32)


def by_date(ref, block):
    return jnp.concatenate([ref[pl.ds(date, EDGE, stride=block), :] for date in range(block)], axis=0)


def square(rows, step, row):
    real, imag = rows[step, 0, row], rows[step, 1, row]
    return real * real + imag * imag


def products(first, second, step, date, which):
    real, imag = {}, {}
    for row in which:
        second_re, second_im = second[step, 0, row], second[step, 1, row]
        first_re = jnp.broadcast_to(first[0, 0, row, pl.ds(date, 1), :], second_re.shape)
        first_im = jnp.broadcast_to(first[0, 1, row, pl.ds(date, 1), :], second_re.shape)
        real[row] = first_re * second_re + first_im * second_im
        imag[row] = first_im * second_re - first_re * second_im
    return real, imag


def window_sums(rows, start, stop):
    last = start + 2 * row_reach
    tails = {last: rows[last]}
    for row in range(last - 1, start - 1, -1):
        tails[row] = tails[row + 1] + rows[row]
    sums, head = [tails[start]], None
    for row in range(start + 1, stop):
        new = rows[row + 2 * row_reach]
        head = new if head is None else head + new
        sums.append(tails[row] + head)
    return sums


def inner_sums(rows, count):
    last = 2 * row_reach
    tails = {last: rows[last]}
    for row in range(last - 1, row_reach - 1, -1):
        tails[row] = tails[row + 1] + rows[row]
    sums, head = [tails[row_reach]], None
    for row in range(1, count):
        new = rows[row + last]
        head = new if head is None else head + new
        sums.append(tails[max(row, row_reach)] + head)
    return sums


def date_weight(first, second, row, date, block):
    return jnp.broadcast_to(first[0, pl.ds(row * block + date, 1), :], (block, second.shape[-1])) * second[pl.ds(row * block, block), :]


def coherence_kernel(
    boxed, staged_before, above, rows, partial, partial_power, weights, band, out, staged, top, found, done,
):
    block, height, breadth = out.shape[3:]

    def copy_boxed(step):
        return pltpu.make_async_copy(
            boxed.at[step], out.at[:, step, :, :, pl.ds(EDGE, height - EDGE), :], done)

    for step in range(SHIFTS):
        copy_boxed(step).start()
    which = range(row_reach)
    above = above.reshape(SHIFTS, 2, block * EDGE, breadth)
    staged_rows = staged.reshape(SHIFTS, 2, block, block * EDGE, breadth)

    for part in range(2):
        for row in which:
            top[0, part, row] = above[0, part, pl.ds(EDGE - row_reach + row, block, stride=EDGE), :]

    def with_top(values, inner):
        tails = [values[row_reach - 1]]
        for row in reversed(which[:-1]):
            tails.insert(0, tails[0] + values[row])
        return [tails[row] + inner[row * block:(row + 1) * block, :] for row in which]

    power = with_top({row: square(top, 0, row) for row in which}, partial_power)
    power = box_columns(jnp.concatenate(power, axis=0), band[...])
    size = block // 2

    def copy_out(step, half):
        dates = pl.ds(half * size, size)
        return pltpu.make_async_copy(
            staged.at[step, :, dates], out.at[:, step, dates, :, pl.ds(0, EDGE), :], done)

    def begin(step, half):
        upper = []
        for date in range(half * size, (half + 1) * size):
            both = products(top, rows if step else top, step, date, which)
            for part, values in enumerate(both):
                upper += with_top(values, partial.at[step, date, part])
        return box_columns(jnp.concatenate(upper, axis=0), band[...])

    def end(step, half, columns):
        for date in range(size):
            for row in which:
                weight = date_weight(found, weights.at[step] if step else found.at[0], row, half * size + date, block)
                for part in range(2):
                    at = ((date * 2 + part) * row_reach + row) * block
                    rows_of = pl.ds(row, block, stride=EDGE)
                    staged_rows[step, part, half * size + date, rows_of, :] = columns[at:at + block] * weight
        copy_out(step, half).start()

    pieces = [(step, half) for step in range(SHIFTS) for half in range(2)]
    begun = None
    for piece in pieces:
        columns = begin(*piece)
        if begun is None:
            found[0] = lax.rsqrt(power)
        else:
            end(*begun)
        begun = (*piece, columns)
    end(*begun)

    pltpu.make_async_copy(out, out, done).wait()


def coherence(height, boxed, staged, *values):
    block, breadth = staged.shape[2], staged.shape[5]
    vmem = pl.BlockSpec(memory_space=pltpu.VMEM)
    return pl.pallas_call(
        coherence_kernel,
        out_shape=(
            pltpu.HBM((2, SHIFTS, block, block, height, breadth), jnp.float32),
            jax.ShapeDtypeStruct(staged.shape, jnp.float32),
        ),
        in_specs=[vmem] * (len(values) + 2),
        out_specs=(pl.BlockSpec(memory_space=pltpu.HBM), vmem),
        scratch_shapes=[
            pltpu.VMEM((1, 2, row_reach, block, breadth), jnp.float32),
            pltpu.VMEM((1, row_reach * block, breadth), jnp.float32),
            pltpu.SemaphoreType.DMA,
        ],
        input_output_aliases={1: 1},
        compiler_params=pltpu.CompilerParams(vmem_limit_bytes=4 << 20),
        name="coherence",
    )(boxed, staged, *values)[0]


def solution(mesh):
    def on_device(acquired):
        return coherence(acquired.shape[2], *exchange(acquired, mesh.shape["date"], mesh.shape["tile"]))

    in_specs = (P(None, "date", ("groups", "tile"), None),)
    out_specs = P(None, None, "date", None, ("groups", "tile"), None)
    return jax.shard_map(
        on_device, mesh=mesh, in_specs=in_specs, out_specs=out_specs, check_vma=False
    )
```
